32 devices in a mesh: seq: 8 (over y, x, core), chan: 4 (over z).
Axes of the slice: x: 2, y: 2, z: 4, core: 2. Of those that a mesh axis runs over, the one named last changes fastest.
Arguments:
- stream: float32 [6144, 4096], P('seq', 'chan'), may hold values from -6 to 6
- short_gate_pre: float32 [6144, 4096], P('seq', 'chan'), may hold values from -6 to 6
- short_gate_post: float32 [6144, 4096], P('seq', 'chan'), may hold values from -6 to 6
- short_filter: float32 [128, 4096], P(None, 'chan'), may hold values from -0.5 to 0.5
- long_gate_pre: float32 [6144, 4096], P('seq', 'chan'), may hold values from -6 to 6
- long_gate_post: float32 [6144, 4096], P('seq', 'chan'), may hold values from -6 to 6
- long_filter: float32 [4096, 6144], P('chan', 'seq'), may hold values from -0.078125 to 0.078125
- queries: float32 [6144, 4096], P('seq', 'chan'), may hold values from -8 to 8
- key_vectors: float32 [6144, 4096], P('seq', 'chan'), may hold values from -8 to 8
- head_reach: int32 [32], P('chan'), may hold values from 1 to 3
- out_weight: float32 [4096, 4096], P('seq', 'chan'), may hold values from -0.09375 to 0.09375
Outputs:
- hyena_out: float32 [6144, 4096], P('seq', 'chan')
- mixed: float32 [6144, 4096], P('seq', 'chan')
The draws below stay inside these ranges and needn't reach their ends.
Inputs may be any that keep to these rules, and one draw needn't show every extreme that they name: Head h reads its own block and the head_reach[h] blocks of 768 tokens before it.
All inputs are finite; a program needn't handle non-finite values.
Results may differ from the reference program's by a relative error of at most 0.0003.
Values sent between devices are 32-bit elements; how exact they have to be, the bound alone decides.
No kernel may reach another device: no remote copies, remote signals or barrier semaphores. Data moves between devices by JAX's collectives and lax.ppermute only.
A program may use at most 256 MiB of HBM per device.

```python
import jax
import jax.numpy as jnp
from jax import lax

D = 4096
HEADS = 32
HEAD_DIM = 128
TAPS = 128
REACH = 3
L_DEV = 768
WINDOW_TOKENS = 6144


def drawn_pair(key):
    base_offset = jax.random.fold_in(key, 11)
    random_query_stream, random_key_stream = jax.random.split(base_offset, 2)
    complete_shape = (WINDOW_TOKENS, D)
    query_part = 1.5 * jnp.clip(jax.random.normal(random_query_stream, complete_shape, jnp.float32), -4.0, 4.0)
    key_portion = 1.5 * jnp.clip(jax.random.normal(random_key_stream, complete_shape, jnp.float32), -4.0, 4.0)
    return (query_part, key_portion)


def draw_queries(key, part):
    return drawn_pair(key)[0]


def draw_key_vectors(key, part):
    return drawn_pair(key)[1]


def plant(values, own_key, low, largest):
    longest = values.shape.index(max(values.shape))
    spots = []
    for shift in (0, 1):
        where = [jax.random.randint(jax.random.fold_in(own_key, axis), (), 0, length) for axis, length in enumerate(values.shape)]
        where[longest] = (where[longest] + shift) % values.shape[longest]
        spots.append(tuple(where))
    return values.at[spots[0]].set(low).at[spots[1]].set(largest)


def level_of(own_key, shape, shards, low, largest):
    gain, own = 1.0, jax.random.fold_in(own_key, 6)
    for dim, parts in shards:
        heights = jnp.exp(jax.random.uniform(jax.random.fold_in(own, dim), (parts,), jnp.float32, low / len(shards), largest / len(shards)))
        gain = gain * jnp.repeat(heights, shape[dim] // parts).reshape([-1 if axis == dim else 1 for axis in range(len(shape))])
    return gain


def centred(own_key, shape, scale, limit, cuts=(), kind=jnp.bfloat16):
    values = scale * jax.random.normal(own_key, shape, jnp.float32)
    if cuts:
        values = values * level_of(own_key, shape, cuts, -0.22, 0.18)
    return jnp.clip(values, -limit, limit).astype(kind)


def setup_inputs(seed: int = 0) -> dict:
    splits = jax.random.split(jax.random.key(seed), 12)
    return {
        "stream": centred(splits[0], (WINDOW_TOKENS, D), 1.0, 6.0, ((0, 8), (1, 4)), jnp.float32),
        "short_gate_pre": centred(splits[1], (WINDOW_TOKENS, D), 1.0, 6.0, ((0, 8), (1, 4)), jnp.float32),
        "short_gate_post": centred(splits[2], (WINDOW_TOKENS, D), 1.0, 6.0, ((0, 8), (1, 4)), jnp.float32),
        "short_filter": centred(splits[3], (TAPS, D), TAPS ** -0.5, 0.5, ((1, 4),), jnp.float32),
        "long_gate_pre": centred(splits[4], (WINDOW_TOKENS, D), 1.0, 6.0, ((0, 8), (1, 4)), jnp.float32),
        "long_gate_post": centred(splits[5], (WINDOW_TOKENS, D), 1.0, 6.0, ((0, 8), (1, 4)), jnp.float32),
        "long_filter": centred(splits[6], (D, WINDOW_TOKENS), WINDOW_TOKENS ** -0.5, 0.078125, ((0, 4), (1, 8)), jnp.float32),
        "queries": draw_queries(jax.random.fold_in(splits[11], 71), 0),
        "key_vectors": draw_key_vectors(jax.random.fold_in(splits[11], 71), 0),
        "head_reach": plant(jax.random.randint(splits[9], (HEADS,), 1, REACH + 1), jax.random.fold_in(splits[9], 1), 1, REACH).astype(jnp.int32),
        "out_weight": centred(splits[10], (D, D), D ** -0.5, 0.09375, ((0, 8), (1, 4)), jnp.float32),
    }


def short_convolve(short_in, taps):
    length = short_in.shape[0]
    padding = jnp.zeros((TAPS - 1, short_in.shape[1]), dtype=short_in.dtype)
    extended = jnp.concatenate([padding, short_in], axis=0)

    def add_tap(index, total):
        start = (TAPS - 1 - index).astype(jnp.int32)
        window = lax.dynamic_slice_in_dim(extended, start, length, 0)
        row = lax.dynamic_slice_in_dim(taps, index.astype(jnp.int32), 1, 0)
        return total + row * window
    return lax.fori_loop(jnp.int32(0), jnp.int32(TAPS), add_tap, jnp.zeros(short_in.shape, dtype=short_in.dtype))

def long_convolve(long_in, long_filter):
    length = long_in.shape[0]
    block = min(D, 256)
    signal = long_in.T.reshape(D // block, block, length)
    kernel = long_filter.reshape(D // block, block, length)

    def one_group(pieces):
        signal_part, kernel_part = pieces
        spectrum = jnp.fft.rfft(signal_part, n=2 * length, axis=1) * jnp.fft.rfft(kernel_part, n=2 * length, axis=1)
        return jnp.fft.irfft(spectrum, n=2 * length, axis=1)[:, :length]
    result = lax.map(one_group, (signal, kernel))
    return result.reshape(D, length).T

def reference(stream, short_gate_pre, short_gate_post, short_filter, long_gate_pre, long_gate_post, long_filter, queries, key_vectors, head_reach, out_weight):
    length = stream.shape[0]
    short_in = short_gate_pre * stream
    short_conv = short_convolve(short_in, short_filter)
    short_out = stream + short_gate_post * short_conv
    long_in = long_gate_pre * short_out
    long_conv = long_convolve(long_in, long_filter)
    hyena_out = short_out + long_gate_post * long_conv
    front = jnp.zeros((REACH * L_DEV, D), dtype=stream.dtype)
    keys_padded = jnp.concatenate([front, key_vectors], axis=0)
    values_padded = jnp.concatenate([front, hyena_out], axis=0)
    window = (REACH + 1) * L_DEV
    column = jnp.arange(window, dtype=jnp.int32)
    distance = REACH - column // L_DEV
    inner_pos = column % L_DEV
    row_pos = jnp.arange(L_DEV, dtype=jnp.int32)

    def one_block(index):
        offset = (index * L_DEV).astype(jnp.int32)
        query_block = lax.dynamic_slice_in_dim(queries, offset, L_DEV, 0).reshape(L_DEV, HEADS, HEAD_DIM)
        key_block = lax.dynamic_slice_in_dim(keys_padded, offset, window, 0).reshape(window, HEADS, HEAD_DIM)
        value_block = lax.dynamic_slice_in_dim(values_padded, offset, window, 0).reshape(window, HEADS, HEAD_DIM)
        scores = jnp.einsum('qhd,khd->hqk', query_block, key_block, precision=lax.Precision.HIGHEST) / jnp.sqrt(jnp.float32(HEAD_DIM)).astype(stream.dtype)
        allowed = (distance[None, None, :] <= head_reach[:, None, None]) & (index - distance >= 0)[None, None, :]
        allowed = allowed & ((distance > 0)[None, None, :] | (inner_pos[None, None, :] <= row_pos[None, :, None]))
        masked = jnp.where(allowed, scores, -jnp.inf)
        probs = jax.nn.softmax(masked, axis=2)
        output = jnp.einsum('hqk,khd->qhd', probs, value_block, precision=lax.Precision.HIGHEST)
        return output.reshape(L_DEV, D)
    attended = lax.map(one_block, jnp.arange(length // L_DEV, dtype=jnp.int32)).reshape(length, D)
    mixed = jnp.dot(attended, out_weight, precision=lax.Precision.HIGHEST)
    return (hyena_out, mixed)
```

```python
import functools
import math

import jax
import jax.numpy as jnp
import numpy as np
from jax import lax
from jax.experimental import pallas as pl
from jax.experimental.pallas import tpu as pltpu
from jax.sharding import PartitionSpec as P

HEAD_DIM = 128
REACH = 3
INNER = 128
SUB = 8
CHUNKS = 2

F32 = jnp.float32
BF16 = jnp.bfloat16
masked_low = -1e30
VMEM_CAP = 58 * 1024 * 1024


def halves(x):
    hi = x.astype(BF16)
    lo = (x - hi.astype(F32)).astype(BF16)
    return hi, lo


def const_halves(x):
    x = np.asarray(x, np.float32)
    hi = x.astype(BF16)
    lo = (x - hi.astype(np.float32)).astype(BF16)
    return hi, lo


def mm(a, b):
    return jnp.dot(a, b, preferred_element_type=F32)


def mm3(a_hi, a_lo, b):
    b_hi, b_lo = halves(b)
    return mm(a_hi, b_hi) + (mm(a_lo, b_hi) + mm(a_hi, b_lo))


@functools.lru_cache(None)
def short_tables(taps):
    size = 2 * taps
    freq = 2.0 * np.pi * (np.arange(taps) + 0.5) / size
    angle = freq[:, None] * np.arange(size)[None, :]
    forward = np.concatenate([np.cos(angle), -np.sin(angle)], axis=0)
    back = angle[:, taps:].T
    inverse = np.concatenate([np.cos(back), -np.sin(back)], axis=1) * (2.0 / size)
    return const_halves(forward) + const_halves(inverse)


def short_kernel(
    f_hi, f_lo, g_hi, g_lo, halo, stream, pre, post, taps_ref, long_pre, out_ref, in_ref
):
    taps = taps_ref.shape[0]
    group = in_ref.shape[2]
    spec = mm3(f_hi[:, :taps], f_lo[:, :taps], taps_ref[...])
    h_re, h_im = spec[:taps], spec[taps:]
    before = halo[...]
    for block in range(stream.shape[0] // taps):
        rows = pl.ds(block * taps, taps)
        signal = stream[rows, :]
        here = pre[rows, :] * signal
        window = jnp.concatenate([before, here], axis=0)
        before = here
        x = mm3(f_hi[...], f_lo[...], window)
        x_re, x_im = x[:taps], x[taps:]
        z = jnp.concatenate([x_re * h_re - x_im * h_im, x_re * h_im + x_im * h_re], axis=0)
        conv = mm3(g_hi[...], g_lo[...], z)
        short_out = signal + post[rows, :] * conv
        out_ref[rows, :] = short_out
        long_in = long_pre[rows, :] * short_out
        for g in range(in_ref.shape[0]):
            in_ref[g, rows, :] = long_in[:, g * group : (g + 1) * group]


def short_stage(halo, stream, pre, post, taps, long_pre, parts):
    length, width = stream.shape
    taps_n = taps.shape[0]
    tile = min(width, 256)
    group = width // parts
    tables = short_tables(taps_n)
    wide = pl.BlockSpec((length, tile), lambda i: (0, i))
    narrow = pl.BlockSpec((taps_n, tile), lambda i: (0, i))
    fixed = [pl.BlockSpec(t.shape, lambda i: (0, 0)) for t in tables]
    return pl.pallas_call(
        short_kernel,
        grid=(width // tile,),
        in_specs=fixed + [narrow, wide, wide, wide, narrow, wide],
        out_specs=[wide, pl.BlockSpec((tile // group, length, group), lambda i: (i, 0, 0))],
        out_shape=[
            jax.ShapeDtypeStruct((length, width), F32),
            jax.ShapeDtypeStruct((parts, length, group), F32),
        ],
        compiler_params=pltpu.CompilerParams(vmem_limit_bytes=VMEM_CAP),
        name="short_stage",
    )(*tables, halo, stream, pre, post, taps, long_pre)


@functools.lru_cache(None)
def long_tables(length):
    outer = length // INNER
    k1 = np.arange(outer) + 0.25
    sub = np.arange(SUB)
    phase = (
        k1[:, None, None] * np.arange(outer)[None, :, None] / outer
        + k1[:, None, None] * sub[None, None, :] / length
    )
    angle = 2.0 * np.pi * phase
    eye = np.eye(SUB)

    def spread(values):
        full = np.einsum("knr,rs->krns", values, eye)
        return full.reshape(outer * SUB, outer * SUB)

    first = np.concatenate([spread(np.cos(angle)), spread(-np.sin(angle))], axis=0)
    last = np.concatenate([spread(np.cos(angle)).T, spread(-np.sin(angle)).T], axis=1) / length
    inner = 2.0 * np.pi * np.outer(np.arange(INNER), np.arange(INNER)) / INNER
    c, s = np.cos(inner), np.sin(inner)
    middle = np.block([[c, s], [-s, c]])
    unmiddle = np.block([[c, -s], [s, c]])
    turn = 2.0 * np.pi * k1[None, :] * (SUB * np.arange(INNER // SUB))[:, None] / length
    scal_re = np.cos(turn).astype(np.float32)
    scal_im = np.sin(turn).astype(np.float32)
    return (
        const_halves(first),
        const_halves(last),
        const_halves(middle),
        const_halves(unmiddle),
        scal_re,
        scal_im,
    )


def forward_outer(x_ref, w_hi, w_lo, t_re, t_im, work):
    outer = x_ref.shape[0]
    lanes = x_ref.shape[2]

    def pair(i, carry):
        tiles = [
            x_ref[:, pl.ds(pl.multiple_of((2 * i + u) * SUB, SUB), SUB), :].reshape(
                outer * SUB, lanes
            )
            for u in range(2)
        ]
        out = mm3(w_hi[...], w_lo[...], jnp.concatenate(tiles, axis=1))
        for u in range(2):
            j = 2 * i + u
            row = pl.multiple_of(j * SUB, SUB)
            for k in range(outer):
                re = out[k * SUB : (k + 1) * SUB, u * lanes : (u + 1) * lanes]
                im = out[(outer + k) * SUB : (outer + k + 1) * SUB, u * lanes : (u + 1) * lanes]
                c, s = t_re[j, k], t_im[j, k]
                work[k, pl.ds(row, SUB), :] = re * c + im * s
                work[k, pl.ds(pl.multiple_of(INNER + row, SUB), SUB), :] = im * c - re * s
        return carry

    lax.fori_loop(0, INNER // SUB // 2, pair, 0)


def filter_kernel(w_hi, w_lo, b_hi, b_lo, t_re, t_im, filt, spec, x_ref, work):
    per = filt.shape[2] // INNER

    def turn(s, carry):
        for a in range(per):
            x_ref[per * s + a] = filt[s, :, a * INNER : (a + 1) * INNER].T
        return carry

    lax.fori_loop(0, filt.shape[0], turn, 0)
    forward_outer(x_ref, w_hi, w_lo, t_re, t_im, work)
    lanes = x_ref.shape[2]

    def inner(i, carry):
        both = jnp.concatenate([work[2 * i], work[2 * i + 1]], axis=1)
        out = mm3(b_hi[...], b_lo[...], both)
        spec[2 * i] = out[:, :lanes]
        spec[2 * i + 1] = out[:, lanes:]
        return carry

    lax.fori_loop(0, work.shape[0] // 2, inner, 0)


def signal_kernel(
    w_hi, w_lo, v_hi, v_lo, b_hi, b_lo, u_hi, u_lo, t_re, t_im, x_ref, spec, out_ref, work
):
    outer = x_ref.shape[0]
    lanes = x_ref.shape[2]
    forward_outer(x_ref, w_hi, w_lo, t_re, t_im, work)

    def inner(i, carry):
        both = jnp.concatenate([work[2 * i], work[2 * i + 1]], axis=1)
        x = mm3(b_hi[...], b_lo[...], both)
        h = jnp.concatenate([spec[2 * i], spec[2 * i + 1]], axis=1)
        x_re, x_im, h_re, h_im = x[:INNER], x[INNER:], h[:INNER], h[INNER:]
        z = jnp.concatenate([x_re * h_re - x_im * h_im, x_re * h_im + x_im * h_re], axis=0)
        y = mm3(u_hi[...], u_lo[...], z)
        work[2 * i] = y[:, :lanes]
        work[2 * i + 1] = y[:, lanes:]
        return carry

    lax.fori_loop(0, outer // 2, inner, 0)

    def back(i, carry):
        tiles = []
        for u in range(2):
            j = 2 * i + u
            row = pl.multiple_of(j * SUB, SUB)
            res, ims = [], []
            for k in range(outer):
                re = work[k, pl.ds(row, SUB), :]
                im = work[k, pl.ds(pl.multiple_of(INNER + row, SUB), SUB), :]
                c, s = t_re[j, k], t_im[j, k]
                res.append(re * c - im * s)
                ims.append(re * s + im * c)
            tiles.append(jnp.concatenate(res + ims, axis=0))
        out = mm3(v_hi[...], v_lo[...], jnp.concatenate(tiles, axis=1))
        for u in range(2):
            row = pl.multiple_of((2 * i + u) * SUB, SUB)
            part = out[:, u * lanes : (u + 1) * lanes].reshape(outer, SUB, lanes)
            out_ref[:, pl.ds(row, SUB), :] = part
        return carry

    lax.fori_loop(0, INNER // SUB // 2, back, 0)


def vmem_spec():
    return pl.BlockSpec(memory_space=pltpu.VMEM)


def smem_spec():
    return pl.BlockSpec(memory_space=pltpu.SMEM)


def filter_stage(filt, length):
    first, _, middle, _, t_re, t_im = long_tables(length)
    outer = length // INNER
    lanes = filt.shape[1]
    return pl.pallas_call(
        filter_kernel,
        in_specs=[vmem_spec()] * 4 + [smem_spec()] * 2 + [vmem_spec()],
        out_specs=vmem_spec(),
        out_shape=jax.ShapeDtypeStruct((outer, 2 * INNER, lanes), F32),
        scratch_shapes=[
            pltpu.VMEM((outer, INNER, lanes), F32),
            pltpu.VMEM((outer, 2 * INNER, lanes), F32),
        ],
        compiler_params=pltpu.CompilerParams(vmem_limit_bytes=VMEM_CAP),
        name="filter_stage",
    )(*first, *middle, t_re, t_im, filt)


def signal_stage(signal, spec):
    outer, _, lanes = signal.shape
    first, last, middle, unmiddle, t_re, t_im = long_tables(outer * INNER)
    return pl.pallas_call(
        signal_kernel,
        in_specs=[vmem_spec()] * 8 + [smem_spec()] * 2 + [vmem_spec()] * 2,
        out_specs=vmem_spec(),
        out_shape=jax.ShapeDtypeStruct(signal.shape, F32),
        scratch_shapes=[pltpu.VMEM((outer, 2 * INNER, lanes), F32)],
        compiler_params=pltpu.CompilerParams(vmem_limit_bytes=VMEM_CAP),
        name="signal_stage",
    )(*first, *last, *middle, *unmiddle, t_re, t_im, signal, spec)


def angle_table(row_count, col_count, modulus):
    product = (
        lax.iota(jnp.int32, row_count)[:, None] * lax.iota(jnp.int32, col_count)[None, :] % modulus
    )
    phase = product.astype(F32) * (2.0 * math.pi / modulus)
    return (jnp.cos(phase), jnp.sin(phase))


def plain_long_convolve(signal, kernel):
    high = lax.Precision.HIGHEST
    channels, length = signal.shape
    outer_len = 2 * length // INNER
    half_len = outer_len // 2
    cos_o, sin_o = angle_table(outer_len, half_len, outer_len)
    cos_t, sin_t = angle_table(outer_len, INNER, 2 * length)
    cos_i, sin_i = angle_table(INNER, INNER, INNER)
    stacked = jnp.concatenate([signal, kernel], axis=0).reshape(2 * channels, half_len, INNER)
    real = jnp.einsum("kn,cnq->ckq", cos_o, stacked, precision=high)
    imag = -jnp.einsum("kn,cnq->ckq", sin_o, stacked, precision=high)
    t_re = real * cos_t + imag * sin_t
    t_im = imag * cos_t - real * sin_t
    s_re = jnp.dot(t_re, cos_i, precision=high) + jnp.dot(t_im, sin_i, precision=high)
    s_im = jnp.dot(t_im, cos_i, precision=high) - jnp.dot(t_re, sin_i, precision=high)
    x_re, h_re, x_im, h_im = s_re[:channels], s_re[channels:], s_im[:channels], s_im[channels:]
    p_re = x_re * h_re - x_im * h_im
    p_im = x_re * h_im + x_im * h_re
    b_re = jnp.dot(p_re, cos_i, precision=high) - jnp.dot(p_im, sin_i, precision=high)
    b_im = jnp.dot(p_im, cos_i, precision=high) + jnp.dot(p_re, sin_i, precision=high)
    u_re = b_re * cos_t - b_im * sin_t
    u_im = b_re * sin_t + b_im * cos_t
    result = jnp.einsum("kn,ckq->cnq", cos_o, u_re, precision=high) - jnp.einsum(
        "kn,ckq->cnq", sin_o, u_im, precision=high
    )
    return result.reshape(channels, length) / (2.0 * length)


def hyena_kernel(short_out, post, conv, out_ref):
    parts = [conv[g] for g in range(conv.shape[0])]
    here = parts[0] if len(parts) == 1 else jnp.concatenate(parts, axis=1)
    out_ref[...] = short_out[...] + post[...] * here


def hyena_stage(short_out, post, conv):
    length, width = short_out.shape
    parts, _, group = conv.shape
    tile = max(group, 128)
    wide = pl.BlockSpec((length, tile), lambda i: (0, i))
    return pl.pallas_call(
        hyena_kernel,
        grid=(width // tile,),
        in_specs=[
            wide,
            wide,
            pl.BlockSpec((tile // group, length, group), lambda i: (i, 0, 0)),
        ],
        out_specs=wide,
        out_shape=jax.ShapeDtypeStruct((length, width), F32),
        name="hyena_stage",
    )(short_out, post, conv)


def attend_kernel(reach_ref, chip_ref, *refs):
    steps = REACH + 2
    q_ref = refs[0]
    k_refs = refs[1 : 1 + steps]
    v_refs = refs[1 + steps : 1 + 2 * steps]
    out_ref, k_cat, v_cat, top, total, acc = refs[1 + 2 * steps :]
    head, odd, tile = pl.program_id(0), pl.program_id(1), pl.program_id(2)
    dim = q_ref.shape[2]
    rows = q_ref.shape[1]
    length = k_refs[0].shape[0]

    @pl.when((odd == 0) & (tile == 0))
    def _():
        for n in range(steps):
            hi, lo = halves(k_refs[n][...])
            k_cat[n] = jnp.concatenate([hi, hi, lo], axis=1)
            hi, lo = halves(v_refs[n][...])
            v_cat[n] = jnp.concatenate([hi, lo], axis=1)

    scale = math.log2(math.e) / math.sqrt(dim)
    q_hi, q_lo = halves(q_ref[0] * scale)
    q_cat = jnp.concatenate([q_hi, q_lo, q_hi], axis=1)
    reach = reach_ref[head]
    block = 2 * chip_ref[0] + odd

    def scores_of(slot):
        return lax.dot_general(
            q_cat, k_cat[slot], (((1,), (1,)), ((), ())), preferred_element_type=F32
        )

    def weigh(slot, weight):
        w_hi, w_lo = halves(weight)
        both = mm(w_hi, v_cat[slot])
        return both[:, :dim] + both[:, dim:] + mm(w_lo, v_cat[slot][:, :dim])

    own = odd + REACH
    scores = scores_of(own)
    row = tile * rows + lax.broadcasted_iota(jnp.int32, (rows, length), 0)
    col = lax.broadcasted_iota(jnp.int32, (rows, length), 1)
    scores = jnp.where(row >= col, scores, masked_low)
    best = jnp.max(scores, axis=1, keepdims=True)
    weight = jnp.exp2(scores - best)
    top[...] = best
    total[...] = jnp.sum(weight, axis=1, keepdims=True)
    acc[...] = weigh(own, weight)

    for distance in range(1, REACH + 1):

        @pl.when((distance <= reach) & (block >= distance))
        def _():
            slot = own - distance
            scores = scores_of(slot)
            old = top[...]
            best = jnp.maximum(old, jnp.max(scores, axis=1, keepdims=True))
            shrink = jnp.exp2(old - best)
            weight = jnp.exp2(scores - best)
            top[...] = best
            total[...] = total[...] * shrink + jnp.sum(weight, axis=1, keepdims=True)
            acc[...] = acc[...] * shrink + weigh(slot, weight)

    out_ref[0] = acc[...] / total[...]


def attend_stage(reach, chip, queries, keys, values, first_head, heads):
    blocks, length, _ = queries.shape
    rows = min(length, 256)
    steps = REACH + 2
    key_spec = pl.BlockSpec((length, HEAD_DIM), lambda h, b, t, *_: (0, first_head + h))
    value_spec = pl.BlockSpec((length, HEAD_DIM), lambda h, b, t, *_: (0, h))
    return pl.pallas_call(
        attend_kernel,
        grid_spec=pltpu.PrefetchScalarGridSpec(
            num_scalar_prefetch=2,
            grid=(heads, blocks, length // rows),
            in_specs=[pl.BlockSpec((1, rows, HEAD_DIM), lambda h, b, t, *_: (b, t, first_head + h))]
            + [key_spec] * steps
            + [value_spec] * steps,
            out_specs=pl.BlockSpec((1, rows, HEAD_DIM), lambda h, b, t, *_: (b, t, h)),
            scratch_shapes=[
                pltpu.VMEM((steps, length, 3 * HEAD_DIM), BF16),
                pltpu.VMEM((steps, length, 2 * HEAD_DIM), BF16),
                pltpu.VMEM((rows, 1), F32),
                pltpu.VMEM((rows, 1), F32),
                pltpu.VMEM((rows, HEAD_DIM), F32),
            ],
        ),
        out_shape=jax.ShapeDtypeStruct((blocks, length, heads * HEAD_DIM), F32),
        compiler_params=pltpu.CompilerParams(vmem_limit_bytes=VMEM_CAP),
        name="attend_stage",
    )(reach, chip, queries, *keys, *values)


def shards(
    stream,
    short_gate_pre,
    short_gate_post,
    short_filter,
    long_gate_pre,
    long_gate_post,
    long_filter,
    queries,
    key_vectors,
    head_reach,
    out_weight,
):
    length, width = stream.shape
    taps = short_filter.shape[0]
    parts = lax.axis_size("seq")
    group = width // parts
    here = lax.axis_index("seq")
    chip, core = here // 2, here % 2
    half = width // 2
    heads_half = half // HEAD_DIM
    chunks = math.gcd(CHUNKS, heads_half)
    heads_chunk = heads_half // chunks
    part = heads_chunk * HEAD_DIM

    def shift(x, by):
        pairs = [(i, i + by) for i in range(parts) if i + by < parts]
        return lax.ppermute(x, "seq", pairs)

    def swap(x):
        return lax.ppermute(x, "seq", [(i, i ^ 1) for i in range(parts)])

    def both_blocks(x):
        cols = x.shape[1] // 2
        mine = lax.dynamic_slice_in_dim(x, core * cols, cols, 1)
        other = swap(lax.dynamic_slice_in_dim(x, (1 - core) * cols, cols, 1))
        even = jnp.where(core == 0, mine, other)
        odd = jnp.where(core == 0, other, mine)
        return jnp.stack([even, odd])

    def window(pair):
        behind = shift(pair, 2)
        far = shift(pair[1], 4)
        return [far, behind[0], behind[1], pair[0], pair[1]]

    filt = long_filter.reshape(parts, group, length)
    filt = lax.all_to_all(filt, "seq", split_axis=0, concat_axis=0, tiled=True)

    tail = short_gate_pre[length - taps :] * stream[length - taps :]
    halo = shift(tail, 1)
    short_out, long_in = short_stage(
        halo, stream, short_gate_pre, short_gate_post, short_filter, long_gate_pre, parts
    )
    signal = lax.all_to_all(long_in, "seq", split_axis=0, concat_axis=0, tiled=True)

    whole = parts * length
    if group == 128 and whole <= 6144:
        spec = filter_stage(filt, whole)
        conv = signal_stage(signal.reshape(whole // INNER, INNER, group), spec)
        conv = conv.reshape(parts, length, group)
    else:
        conv = plain_long_convolve(
            signal.reshape(whole, group).T, filt.transpose(1, 0, 2).reshape(group, whole)
        ).T.reshape(parts, length, group)
    back = lax.all_to_all(conv, "seq", split_axis=0, concat_axis=0, tiled=True)
    hyena_out = hyena_stage(short_out, long_gate_post, back)

    query_pair = both_blocks(queries)
    keys = window(both_blocks(key_vectors))
    groups = [list(range(c, parts, 2)) for c in range(2)]
    weight = lax.all_gather(out_weight, "seq", axis=0, axis_index_groups=groups)

    reach = lax.dynamic_slice_in_dim(head_reach, core * heads_half, heads_half)
    chip_at = chip[None].astype(jnp.int32)
    mixed = None
    for n in range(chunks):
        cols = jnp.concatenate(
            [hyena_out[:, n * part : (n + 1) * part], hyena_out[:, half + n * part : half + (n + 1) * part]],
            axis=1,
        )
        values = window(both_blocks(cols))
        attended = attend_stage(
            lax.dynamic_slice_in_dim(reach, n * heads_chunk, heads_chunk),
            chip_at,
            query_pair,
            keys,
            values,
            n * heads_chunk,
            heads_chunk,
        ).reshape(2 * length, part)
        spread = lax.all_gather(attended, "chan", axis=0)
        product = lax.dot_general(
            spread,
            weight[:, n * part : (n + 1) * part, :],
            (((0, 2), (0, 1)), ((), ())),
            precision=lax.Precision.HIGH,
            preferred_element_type=F32,
        )
        mixed = product if mixed is None else mixed + product
    mixed = mixed.reshape(2, length, width)
    own = lax.dynamic_index_in_dim(mixed, core, 0, keepdims=False)
    mixed = own + swap(lax.dynamic_index_in_dim(mixed, 1 - core, 0, keepdims=False))
    return (hyena_out, mixed)


def solution(mesh):
    return jax.shard_map(
        shards,
        mesh=mesh,
        in_specs=(
            P("seq", "chan"),
            P("seq", "chan"),
            P("seq", "chan"),
            P(None, "chan"),
            P("seq", "chan"),
            P("seq", "chan"),
            P("chan", "seq"),
            P("seq", "chan"),
            P("seq", "chan"),
            P("chan"),
            P("seq", "chan"),
        ),
        out_specs=(P("seq", "chan"), P("seq", "chan")),
        check_vma=False,
    )
```

```python
import functools
import math

import jax
import jax.numpy as jnp
import numpy as np
from jax import lax
from jax.experimental import pallas as pl
from jax.experimental.pallas import tpu as pltpu
from jax.sharding import PartitionSpec as P

HEAD_DIM = 128
REACH = 3
INNER = 128
SUB = 8


F32 = jnp.float32
BF16 = jnp.bfloat16
masked_low = -1e30
VMEM_CAP = 58 * 1024 * 1024


def halves(x):
    hi = x.astype(BF16)
    lo = (x - hi.astype(F32)).astype(BF16)
    return hi, lo


def const_halves(x):
    x = np.asarray(x, np.float32)
    hi = x.astype(BF16)
    lo = (x - hi.astype(np.float32)).astype(BF16)
    return hi, lo


def mm(a, b):
    return jnp.dot(a, b, preferred_element_type=F32)


def mm3(a_hi, a_lo, b):
    b_hi, b_lo = halves(b)
    left = jnp.concatenate([a_hi, a_lo, a_hi], axis=1)
    return mm(left, jnp.concatenate([b_hi, b_hi, b_lo], axis=0))


@functools.lru_cache(None)
def short_tables(taps):
    size = 2 * taps
    freq = 2.0 * np.pi * (np.arange(taps) + 0.5) / size
    angle = freq[:, None] * np.arange(size)[None, :]
    forward = np.concatenate([np.cos(angle), -np.sin(angle)], axis=0)
    back = angle[:, taps:].T
    inverse = np.concatenate([np.cos(back), -np.sin(back)], axis=1) * (2.0 / size)
    return const_halves(forward) + const_halves(inverse)


def short_kernel(
    f_hi, f_lo, g_hi, g_lo, halo, stream, pre, post, taps_ref, long_pre, out_ref, in_ref
):
    taps = taps_ref.shape[0]
    group = in_ref.shape[2]
    spec = mm3(f_hi[:, :taps], f_lo[:, :taps], taps_ref[...])
    h_re, h_im = spec[:taps], spec[taps:]
    before = halo[...]
    for block in range(stream.shape[0] // taps):
        rows = pl.ds(block * taps, taps)
        signal = stream[rows, :]
        here = pre[rows, :] * signal
        window = jnp.concatenate([before, here], axis=0)
        before = here
        x = mm3(f_hi[...], f_lo[...], window)
        x_re, x_im = x[:taps], x[taps:]
        z = jnp.concatenate([x_re * h_re - x_im * h_im, x_re * h_im + x_im * h_re], axis=0)
        conv = mm3(g_hi[...], g_lo[...], z)
        short_out = signal + post[rows, :] * conv
        out_ref[rows, :] = short_out
        long_in = long_pre[rows, :] * short_out
        for g in range(in_ref.shape[0]):
            in_ref[g, rows, :] = long_in[:, g * group : (g + 1) * group]


def short_stage(halo, stream, pre, post, taps, long_pre, parts):
    length, width = stream.shape
    taps_n = taps.shape[0]
    tile = min(width, 256)
    group = width // parts
    tables = short_tables(taps_n)
    wide = pl.BlockSpec((length, tile), lambda i: (0, i))
    narrow = pl.BlockSpec((taps_n, tile), lambda i: (0, i))
    fixed = [pl.BlockSpec(t.shape, lambda i: (0, 0)) for t in tables]
    return pl.pallas_call(
        short_kernel,
        grid=(width // tile,),
        in_specs=fixed + [narrow, wide, wide, wide, narrow, wide],
        out_specs=[wide, pl.BlockSpec((tile // group, length, group), lambda i: (i, 0, 0))],
        out_shape=[
            jax.ShapeDtypeStruct((length, width), F32),
            jax.ShapeDtypeStruct((parts, length, group), F32),
        ],
        compiler_params=pltpu.CompilerParams(vmem_limit_bytes=VMEM_CAP),
        name="short_stage",
    )(*tables, halo, stream, pre, post, taps, long_pre)


@functools.lru_cache(None)
def long_tables(length):
    outer = length // INNER
    k1 = np.arange(outer) + 0.25
    sub = np.arange(SUB)
    phase = (
        k1[:, None, None] * np.arange(outer)[None, :, None] / outer
        + k1[:, None, None] * sub[None, None, :] / length
    )
    angle = 2.0 * np.pi * phase
    eye = np.eye(SUB)

    def spread(values):
        full = np.einsum("knr,rs->krns", values, eye)
        return full.reshape(outer * SUB, outer * SUB)

    first = np.concatenate([spread(np.cos(angle)), spread(-np.sin(angle))], axis=0)
    last = np.concatenate([spread(np.cos(angle)).T, spread(-np.sin(angle)).T], axis=1) / length
    inner = 2.0 * np.pi * np.outer(np.arange(INNER), np.arange(INNER)) / INNER
    c, s = np.cos(inner), np.sin(inner)
    middle = np.block([[c, s], [-s, c]])
    unmiddle = np.block([[c, -s], [s, c]])
    turn = 2.0 * np.pi * k1[None, :] * (SUB * np.arange(INNER // SUB))[:, None] / length
    scal_re = np.cos(turn).astype(np.float32)
    scal_im = np.sin(turn).astype(np.float32)
    return (
        const_halves(first),
        const_halves(last),
        const_halves(middle),
        const_halves(unmiddle),
        scal_re,
        scal_im,
    )


def forward_outer(x_ref, w_hi, w_lo, t_re, t_im, work):
    outer = x_ref.shape[0]
    lanes = x_ref.shape[2]

    def pair(i, carry):
        tiles = [
            x_ref[:, pl.ds(pl.multiple_of((2 * i + u) * SUB, SUB), SUB), :].reshape(
                outer * SUB, lanes
            )
            for u in range(2)
        ]
        out = mm3(w_hi[...], w_lo[...], jnp.concatenate(tiles, axis=1))
        for u in range(2):
            j = 2 * i + u
            row = pl.multiple_of(j * SUB, SUB)
            for k in range(outer):
                re = out[k * SUB : (k + 1) * SUB, u * lanes : (u + 1) * lanes]
                im = out[(outer + k) * SUB : (outer + k + 1) * SUB, u * lanes : (u + 1) * lanes]
                c, s = t_re[j, k], t_im[j, k]
                work[k, pl.ds(row, SUB), :] = re * c + im * s
                work[k, pl.ds(pl.multiple_of(INNER + row, SUB), SUB), :] = im * c - re * s
        return carry

    lax.fori_loop(0, INNER // SUB // 2, pair, 0)


def filter_kernel(w_hi, w_lo, b_hi, b_lo, t_re, t_im, filt, spec, x_ref, work):
    per = filt.shape[2] // INNER

    def turn(s, carry):
        for a in range(per):
            x_ref[per * s + a] = filt[s, :, a * INNER : (a + 1) * INNER].T
        return carry

    lax.fori_loop(0, filt.shape[0], turn, 0)
    forward_outer(x_ref, w_hi, w_lo, t_re, t_im, work)
    lanes = x_ref.shape[2]

    def inner(i, carry):
        both = jnp.concatenate([work[2 * i], work[2 * i + 1]], axis=1)
        out = mm3(b_hi[...], b_lo[...], both)
        spec[2 * i] = out[:, :lanes]
        spec[2 * i + 1] = out[:, lanes:]
        return carry

    lax.fori_loop(0, work.shape[0] // 2, inner, 0)


def signal_kernel(
    w_hi, w_lo, v_hi, v_lo, b_hi, b_lo, u_hi, u_lo, t_re, t_im, x_ref, spec, out_ref, work
):
    outer = x_ref.shape[0]
    lanes = x_ref.shape[2]
    forward_outer(x_ref, w_hi, w_lo, t_re, t_im, work)

    def inner(i, carry):
        both = jnp.concatenate([work[2 * i], work[2 * i + 1]], axis=1)
        x = mm3(b_hi[...], b_lo[...], both)
        h = jnp.concatenate([spec[2 * i], spec[2 * i + 1]], axis=1)
        x_re, x_im, h_re, h_im = x[:INNER], x[INNER:], h[:INNER], h[INNER:]
        z = jnp.concatenate([x_re * h_re - x_im * h_im, x_re * h_im + x_im * h_re], axis=0)
        y = mm3(u_hi[...], u_lo[...], z)
        work[2 * i] = y[:, :lanes]
        work[2 * i + 1] = y[:, lanes:]
        return carry

    lax.fori_loop(0, outer // 2, inner, 0)

    def back(i, carry):
        tiles = []
        for u in range(2):
            j = 2 * i + u
            row = pl.multiple_of(j * SUB, SUB)
            res, ims = [], []
            for k in range(outer):
                re = work[k, pl.ds(row, SUB), :]
                im = work[k, pl.ds(pl.multiple_of(INNER + row, SUB), SUB), :]
                c, s = t_re[j, k], t_im[j, k]
                res.append(re * c - im * s)
                ims.append(re * s + im * c)
            tiles.append(jnp.concatenate(res + ims, axis=0))
        out = mm3(v_hi[...], v_lo[...], jnp.concatenate(tiles, axis=1))
        for u in range(2):
            row = pl.multiple_of((2 * i + u) * SUB, SUB)
            part = out[:, u * lanes : (u + 1) * lanes].reshape(outer, SUB, lanes)
            out_ref[:, pl.ds(row, SUB), :] = part
        return carry

    lax.fori_loop(0, INNER // SUB // 2, back, 0)


def vmem_spec():
    return pl.BlockSpec(memory_space=pltpu.VMEM)


def smem_spec():
    return pl.BlockSpec(memory_space=pltpu.SMEM)


def filter_stage(filt, length):
    first, _, middle, _, t_re, t_im = long_tables(length)
    outer = length // INNER
    lanes = filt.shape[1]
    return pl.pallas_call(
        filter_kernel,
        in_specs=[vmem_spec()] * 4 + [smem_spec()] * 2 + [vmem_spec()],
        out_specs=vmem_spec(),
        out_shape=jax.ShapeDtypeStruct((outer, 2 * INNER, lanes), F32),
        scratch_shapes=[
            pltpu.VMEM((outer, INNER, lanes), F32),
            pltpu.VMEM((outer, 2 * INNER, lanes), F32),
        ],
        compiler_params=pltpu.CompilerParams(vmem_limit_bytes=VMEM_CAP),
        name="filter_stage",
    )(*first, *middle, t_re, t_im, filt)


def signal_stage(signal, spec):
    outer, _, lanes = signal.shape
    first, last, middle, unmiddle, t_re, t_im = long_tables(outer * INNER)
    return pl.pallas_call(
        signal_kernel,
        in_specs=[vmem_spec()] * 8 + [smem_spec()] * 2 + [vmem_spec()] * 2,
        out_specs=vmem_spec(),
        out_shape=jax.ShapeDtypeStruct(signal.shape, F32),
        scratch_shapes=[pltpu.VMEM((outer, 2 * INNER, lanes), F32)],
        compiler_params=pltpu.CompilerParams(vmem_limit_bytes=VMEM_CAP),
        name="signal_stage",
    )(*first, *last, *middle, *unmiddle, t_re, t_im, signal, spec)


def angle_table(row_count, col_count, modulus):
    product = (
        lax.iota(jnp.int32, row_count)[:, None] * lax.iota(jnp.int32, col_count)[None, :] % modulus
    )
    phase = product.astype(F32) * (2.0 * math.pi / modulus)
    return (jnp.cos(phase), jnp.sin(phase))


def plain_long_convolve(signal, kernel):
    high = lax.Precision.HIGHEST
    channels, length = signal.shape
    outer_len = 2 * length // INNER
    half_len = outer_len // 2
    cos_o, sin_o = angle_table(outer_len, half_len, outer_len)
    cos_t, sin_t = angle_table(outer_len, INNER, 2 * length)
    cos_i, sin_i = angle_table(INNER, INNER, INNER)
    stacked = jnp.concatenate([signal, kernel], axis=0).reshape(2 * channels, half_len, INNER)
    real = jnp.einsum("kn,cnq->ckq", cos_o, stacked, precision=high)
    imag = -jnp.einsum("kn,cnq->ckq", sin_o, stacked, precision=high)
    t_re = real * cos_t + imag * sin_t
    t_im = imag * cos_t - real * sin_t
    s_re = jnp.dot(t_re, cos_i, precision=high) + jnp.dot(t_im, sin_i, precision=high)
    s_im = jnp.dot(t_im, cos_i, precision=high) - jnp.dot(t_re, sin_i, precision=high)
    x_re, h_re, x_im, h_im = s_re[:channels], s_re[channels:], s_im[:channels], s_im[channels:]
    p_re = x_re * h_re - x_im * h_im
    p_im = x_re * h_im + x_im * h_re
    b_re = jnp.dot(p_re, cos_i, precision=high) - jnp.dot(p_im, sin_i, precision=high)
    b_im = jnp.dot(p_im, cos_i, precision=high) + jnp.dot(p_re, sin_i, precision=high)
    u_re = b_re * cos_t - b_im * sin_t
    u_im = b_re * sin_t + b_im * cos_t
    result = jnp.einsum("kn,ckq->cnq", cos_o, u_re, precision=high) - jnp.einsum(
        "kn,ckq->cnq", sin_o, u_im, precision=high
    )
    return result.reshape(channels, length) / (2.0 * length)


def hyena_kernel(place_ref, short_out, post, conv, out_ref, other_ref, mine_ref):
    parts = [conv[g] for g in range(conv.shape[0])]
    here = parts[0] if len(parts) == 1 else jnp.concatenate(parts, axis=1)
    result = short_out[...] + post[...] * here
    out_ref[...] = result
    step, half = pl.program_id(0), pl.num_programs(0) // 2

    @pl.when(step < half)
    def _():
        other_ref[...] = result

    @pl.when(step >= half)
    def _():
        mine_ref[...] = result


def hyena_stage(place, short_out, post, conv):
    length, width = short_out.shape
    _, _, group = conv.shape
    tile = max(group, 128)
    steps = width // tile
    half = steps // 2

    def col(i, place):
        return lax.rem((1 - place[1]) * half + i, steps)

    wide = pl.BlockSpec((length, tile), lambda i, place: (0, col(i, place)))
    return pl.pallas_call(
        hyena_kernel,
        grid_spec=pltpu.PrefetchScalarGridSpec(
            num_scalar_prefetch=1,
            grid=(steps,),
            in_specs=[
                wide,
                wide,
                pl.BlockSpec(
                    (tile // group, length, group), lambda i, place: (col(i, place), 0, 0)
                ),
            ],
            out_specs=[
                wide,
                pl.BlockSpec((length, tile), lambda i, place: (0, jnp.minimum(i, half - 1))),
                pl.BlockSpec((length, tile), lambda i, place: (0, jnp.maximum(i - half, 0))),
            ],
        ),
        out_shape=[
            jax.ShapeDtypeStruct((length, width), F32),
            jax.ShapeDtypeStruct((length, width // 2), F32),
            jax.ShapeDtypeStruct((length, width // 2), F32),
        ],
        name="hyena_stage",
    )(place, short_out, post, conv)


def attend_kernel(reach_ref, place_ref, *refs, head, names):
    count = len(names)
    q_refs = refs[:2]
    k_refs = dict(zip(names, refs[2 : 2 + count]))
    v_refs = dict(zip(names, refs[2 + count : 2 + 2 * count]))
    other_ref, mine_ref, k_cat, v_cat, top, total, acc = refs[2 + 2 * count :]
    turn = pl.program_id(0)
    core = place_ref[1]
    odd = jnp.where(turn == 0, 1 - core, core)
    length, dim = mine_ref.shape

    def load(ref):
        return ref[0] if len(ref.shape) == 3 else ref[...]

    def ordered(refs):
        first = core == 0
        x = {name: load(ref) for name, ref in refs.items()}
        yield x["far"]
        yield jnp.where(first, x["near_mine"], x["near_other"])
        yield jnp.where(first, x["near_other"], x["near_mine"])
        yield jnp.where(first, x["mine"], x["other"])
        yield jnp.where(first, x["other"], x["mine"])

    @pl.when(turn == 0)
    def _():
        for n, k in enumerate(ordered(k_refs)):
            hi, lo = halves(k.T)
            k_cat[n] = jnp.concatenate([hi, hi, lo], axis=0)
        for n, v in enumerate(ordered(v_refs)):
            hi, lo = halves(v)
            v_cat[n] = jnp.concatenate([hi, lo], axis=1)

    scale = math.log2(math.e) / math.sqrt(dim)
    queries = jnp.where(turn == 0, q_refs[1][...], q_refs[0][...])
    q_hi, q_lo = halves(queries * scale)
    q_cat = jnp.concatenate([q_hi, q_lo, q_hi], axis=1)
    reach = reach_ref[head]
    block = 2 * place_ref[0] + odd
    own = odd + REACH

    def weigh(weight, values):
        w_hi, w_lo = halves(weight)
        both = mm(w_hi, values)
        return both[:, :dim] + both[:, dim:] + mm(w_lo, values[:, :dim])

    tile = min(length, 256)
    for start in range(0, length, tile):
        rows, stop = pl.ds(start, tile), start + tile
        scores = mm(q_cat[start:stop], k_cat[own, :, :stop])
        row = start + lax.broadcasted_iota(jnp.int32, (tile, stop), 0)
        col = lax.broadcasted_iota(jnp.int32, (tile, stop), 1)
        scores = jnp.where(row >= col, scores, masked_low)
        best = jnp.max(scores, axis=1, keepdims=True)
        weight = jnp.exp2(scores - best)
        top[rows, :] = best
        total[rows, :] = jnp.sum(weight, axis=1, keepdims=True)
        acc[rows, :] = weigh(weight, v_cat[own, :stop, :])

    for distance in range(1, REACH + 1):

        @pl.when((distance <= reach) & (block >= distance))
        def _():
            slot = own - distance
            scores = mm(q_cat, k_cat[slot])
            old = top[...]
            best = jnp.maximum(old, jnp.max(scores, axis=1, keepdims=True))
            shrink = jnp.exp2(old - best)
            weight = jnp.exp2(scores - best)
            top[...] = best
            total[...] = total[...] * shrink + jnp.sum(weight, axis=1, keepdims=True)
            acc[...] = acc[...] * shrink + weigh(weight, v_cat[slot])

    result = acc[...] / total[...]

    @pl.when(turn == 0)
    def _():
        other_ref[...] = result

    @pl.when(turn == 1)
    def _():
        mine_ref[...] = result


def attend_stage(reach, place, queries, keys, values, head):
    length = queries[0].shape[0]
    steps = REACH + 2

    def spec_of(x, lead):
        if lead is not None:
            return pl.BlockSpec((1, length, HEAD_DIM), lambda i, *_: (lead, 0, 0))
        at = head if x.shape[1] > HEAD_DIM else 0
        return pl.BlockSpec((length, HEAD_DIM), lambda i, *_: (0, at))

    operands = [(q, None) for q in queries] + list(keys.values()) + list(values.values())
    return pl.pallas_call(
        functools.partial(attend_kernel, head=head, names=tuple(keys)),
        grid_spec=pltpu.PrefetchScalarGridSpec(
            num_scalar_prefetch=2,
            grid=(2,),
            in_specs=[spec_of(*x) for x in operands],
            out_specs=[pl.BlockSpec((length, HEAD_DIM), lambda i, *_: (0, 0))] * 2,
            scratch_shapes=[
                pltpu.VMEM((steps, 3 * HEAD_DIM, length), BF16),
                pltpu.VMEM((steps, length, 2 * HEAD_DIM), BF16),
                pltpu.VMEM((length, 1), F32),
                pltpu.VMEM((length, 1), F32),
                pltpu.VMEM((length, HEAD_DIM), F32),
            ],
        ),
        out_shape=[jax.ShapeDtypeStruct((length, HEAD_DIM), F32)] * 2,
        compiler_params=pltpu.CompilerParams(vmem_limit_bytes=VMEM_CAP),
        name="attend_stage",
    )(reach, place, *[x for x, _ in operands])


def product_kernel(place_ref, *refs, count, added):
    a_refs, w_refs = refs[:count], refs[count : 3 * count]
    rest = refs[3 * count :]
    out_ref, left = rest[-2:]

    @pl.when(pl.program_id(0) == 0)
    def _():
        apart = place_ref[0] ^ place_ref[2]
        for h in range(2):
            pieces = [r[h] for r in a_refs]
            bit = 1
            while bit < count:
                flip = (apart & bit) != 0
                pieces = [jnp.where(flip, pieces[m ^ bit], pieces[m]) for m in range(count)]
                bit *= 2
            hi, lo = halves(jnp.concatenate(pieces, axis=1))
            left[h] = jnp.concatenate([hi, lo, hi], axis=1)

    out = None
    for h in range(2):
        hi, lo = halves(jnp.concatenate([r[...] for r in w_refs[h * count : (h + 1) * count]], axis=0))
        here = mm(left[h], jnp.concatenate([hi, hi, lo], axis=0))
        out = here if out is None else out + here
    out_ref[...] = rest[0][...] + out if added else out


def product_stage(place, pieces, weights, head, total):
    count = len(pieces)
    _, length, part = pieces[0].shape
    width = weights[0].shape[1]
    tile = min(width, 256)
    a_spec = pl.BlockSpec((2, length, part), lambda i, place: (0, 0, 0))
    w_spec = pl.BlockSpec((part, tile), lambda i, place: (head, i))
    out_spec = pl.BlockSpec((length, tile), lambda i, place: (0, i))
    extra = [] if total is None else [total]
    return pl.pallas_call(
        functools.partial(product_kernel, count=count, added=total is not None),
        grid_spec=pltpu.PrefetchScalarGridSpec(
            num_scalar_prefetch=1,
            grid=(width // tile,),
            in_specs=[a_spec] * count + [w_spec] * (2 * count) + [out_spec] * len(extra),
            out_specs=out_spec,
            scratch_shapes=[pltpu.VMEM((2, length, 3 * count * part), BF16)],
        ),
        out_shape=jax.ShapeDtypeStruct((length, width), F32),
        compiler_params=pltpu.CompilerParams(vmem_limit_bytes=VMEM_CAP),
        name="product_stage",
    )(place, *pieces, *weights, *extra)


def shards(
    stream,
    short_gate_pre,
    short_gate_post,
    short_filter,
    long_gate_pre,
    long_gate_post,
    long_filter,
    queries,
    key_vectors,
    head_reach,
    out_weight,
):
    length, width = stream.shape
    taps = short_filter.shape[0]
    parts = lax.axis_size("seq")
    group = width // parts
    here = lax.axis_index("seq")
    chip, core = here // 2, here % 2
    half = width // 2
    heads_half = half // HEAD_DIM
    chips = parts // 2
    planes = lax.axis_size("chan")
    plane = lax.axis_index("chan")
    place = jnp.stack([chip, core, plane]).astype(jnp.int32)

    def send(x, pairs):
        return lax.ppermute(x, "seq", pairs)

    def shift(x, by):
        return send(x, [(i, i + by) for i in range(parts) if i + by < parts])

    def swap(x):
        return send(x, [(i, i ^ 1) for i in range(parts)])

    def both(x):
        cols = x.shape[1] // 2
        other = lax.dynamic_slice_in_dim(x, (1 - core) * cols, cols, 1)
        other = swap(other)
        return lax.dynamic_slice_in_dim(x, core * cols, cols, 1), other

    def cut(x, head):
        return x[:, head * HEAD_DIM : (head + 1) * HEAD_DIM]

    def own_of(mine, other):
        return {"mine": (mine, None), "other": (other, None)}

    def first_window(mine, other):
        near_mine = shift(cut(mine, 0), 2)
        near_other = shift(cut(other, 0), 2)
        far = shift(jnp.where(core == 0, cut(other, 0), cut(mine, 0)), 4)
        near = {"far": (far, None), "near_mine": (near_mine, None), "near_other": (near_other, None)}
        return near | own_of(mine, other)

    def later_windows(mine, other, heads):
        near = jnp.stack([cut(x, head) for head in heads for x in (mine, other)])
        far = jnp.stack([jnp.where(core == 0, cut(other, h), cut(mine, h)) for h in heads])
        near = shift(near, 2)
        far = shift(far, 4)
        return [
            {"far": (far, at), "near_mine": (near, 2 * at), "near_other": (near, 2 * at + 1)}
            | own_of(mine, other)
            for at in range(len(heads))
        ]

    tail = short_gate_pre[length - taps :] * stream[length - taps :]
    halo = shift(tail, 1)
    filt = long_filter.reshape(parts, group, length)
    filt = lax.all_to_all(filt, "seq", split_axis=0, concat_axis=0, tiled=True)
    short_out, long_in = short_stage(
        halo, stream, short_gate_pre, short_gate_post, short_filter, long_gate_pre, parts
    )
    signal = lax.all_to_all(long_in, "seq", split_axis=0, concat_axis=0, tiled=True)

    queries = both(queries)
    key_mine, key_other = both(key_vectors)
    whole = parts * length
    if group == 128 and whole <= 6144:
        spec = filter_stage(filt, whole)
        key_mine, key_other, spec = lax.optimization_barrier((key_mine, key_other, spec))
        conv = signal_stage(signal.reshape(whole // INNER, INNER, group), spec)
        conv = conv.reshape(parts, length, group)
    else:
        conv = plain_long_convolve(
            signal.reshape(whole, group).T, filt.transpose(1, 0, 2).reshape(group, whole)
        ).T.reshape(parts, length, group)
    back = lax.all_to_all(conv, "seq", split_axis=0, concat_axis=0, tiled=True)
    hyena_out, value_other, value_mine = hyena_stage(place, short_out, long_gate_post, back)
    value_other = swap(value_other)

    reach = lax.dynamic_slice_in_dim(head_reach, core * heads_half, heads_half)
    weights = None
    mixed = None
    key_windows = [first_window(key_mine, key_other)]
    for n in range(1, heads_half):
        key_windows += later_windows(key_mine, key_other, [n])
    for n in range(heads_half):
        keys = key_windows[n]
        if n == 0:
            values = first_window(value_mine, value_other)
        else:
            values = later_windows(value_mine, value_other, [n])[0]
        other, mine = attend_stage(reach, place, queries, keys, values, n)
        if n == 0:
            out_weight, mine = lax.optimization_barrier((out_weight, mine))
            weights = [out_weight]
            for m in range(1, chips):
                weights.append(send(out_weight, [(i, i ^ (2 * m)) for i in range(parts)]))
            for m in range(chips):
                weights.append(swap(weights[m]))
        piece = jnp.stack([mine, swap(other)])
        pieces = [piece]
        for m in range(1, planes):
            pieces.append(lax.ppermute(piece, "chan", [(i, i ^ m) for i in range(planes)]))
        mixed = product_stage(place, pieces, weights, n, mixed)
    return (hyena_out, mixed)


def solution(mesh):
    return jax.shard_map(
        shards,
        mesh=mesh,
        in_specs=(
            P("seq", "chan"),
            P("seq", "chan"),
            P("seq", "chan"),
            P(None, "chan"),
            P("seq", "chan"),
            P("seq", "chan"),
            P("chan", "seq"),
            P("seq", "chan"),
            P("seq", "chan"),
            P("chan"),
            P("seq", "chan"),
        ),
        out_specs=(P("seq", "chan"), P("seq", "chan")),
        check_vma=False,
    )
```

```python
import functools
import math

import jax
import jax.numpy as jnp
import numpy as np
from jax import lax
from jax.experimental import pallas as pl
from jax.experimental.pallas import tpu as pltpu
from jax.sharding import PartitionSpec as P

HEAD_DIM = 128
REACH = 3
INNER = 128
SUB = 8


F32 = jnp.float32
BF16 = jnp.bfloat16
masked_low = -1e30
VMEM_CAP = 58 * 1024 * 1024


def halves(x):
    hi = x.astype(BF16)
    lo = (x - hi.astype(F32)).astype(BF16)
    return hi, lo


def const_halves(x):
    x = np.asarray(x, np.float32)
    hi = x.astype(BF16)
    lo = (x - hi.astype(np.float32)).astype(BF16)
    return hi, lo


def mm(a, b):
    return jnp.dot(a, b, preferred_element_type=F32)


def mm3(a_hi, a_lo, b):
    b_hi, b_lo = halves(b)
    left = jnp.concatenate([a_hi, a_lo, a_hi], axis=1)
    return mm(left, jnp.concatenate([b_hi, b_hi, b_lo], axis=0))


@functools.lru_cache(None)
def short_tables(taps):
    size = 2 * taps
    freq = 2.0 * np.pi * (np.arange(taps) + 0.5) / size
    angle = freq[:, None] * np.arange(size)[None, :]
    forward = np.concatenate([np.cos(angle), -np.sin(angle)], axis=0)
    back = angle[:, taps:].T
    inverse = np.concatenate([np.cos(back), -np.sin(back)], axis=1) * (2.0 / size)
    return const_halves(forward) + const_halves(inverse)


def short_kernel(
    f_hi, f_lo, g_hi, g_lo, halo, stream, pre, post, taps_ref, long_pre, out_ref, in_ref
):
    taps = taps_ref.shape[0]
    group = in_ref.shape[2]
    spec = mm3(f_hi[:, :taps], f_lo[:, :taps], taps_ref[...])
    h_re, h_im = spec[:taps], spec[taps:]
    before = halo[...]
    for block in range(stream.shape[0] // taps):
        rows = pl.ds(block * taps, taps)
        signal = stream[rows, :]
        here = pre[rows, :] * signal
        window = jnp.concatenate([before, here], axis=0)
        before = here
        x = mm3(f_hi[...], f_lo[...], window)
        x_re, x_im = x[:taps], x[taps:]
        z = jnp.concatenate([x_re * h_re - x_im * h_im, x_re * h_im + x_im * h_re], axis=0)
        conv = mm3(g_hi[...], g_lo[...], z)
        short_out = signal + post[rows, :] * conv
        out_ref[rows, :] = short_out
        long_in = long_pre[rows, :] * short_out
        for g in range(in_ref.shape[0]):
            in_ref[g, rows, :] = long_in[:, g * group : (g + 1) * group]


def short_stage(halo, stream, pre, post, taps, long_pre, parts):
    length, width = stream.shape
    taps_n = taps.shape[0]
    tile = min(width, 256)
    group = width // parts
    tables = short_tables(taps_n)
    wide = pl.BlockSpec((length, tile), lambda i: (0, i))
    narrow = pl.BlockSpec((taps_n, tile), lambda i: (0, i))
    fixed = [pl.BlockSpec(t.shape, lambda i: (0, 0)) for t in tables]
    return pl.pallas_call(
        short_kernel,
        grid=(width // tile,),
        in_specs=fixed + [narrow, wide, wide, wide, narrow, wide],
        out_specs=[wide, pl.BlockSpec((tile // group, length, group), lambda i: (i, 0, 0))],
        out_shape=[
            jax.ShapeDtypeStruct((length, width), F32),
            jax.ShapeDtypeStruct((parts, length, group), F32),
        ],
        compiler_params=pltpu.CompilerParams(vmem_limit_bytes=VMEM_CAP),
        name="short_stage",
    )(*tables, halo, stream, pre, post, taps, long_pre)


@functools.lru_cache(None)
def long_tables(length):
    outer = length // INNER
    k1 = np.arange(outer) + 0.25
    sub = np.arange(SUB)
    phase = (
        k1[:, None, None] * np.arange(outer)[None, :, None] / outer
        + k1[:, None, None] * sub[None, None, :] / length
    )
    angle = 2.0 * np.pi * phase
    eye = np.eye(SUB)

    def spread(values):
        full = np.einsum("knr,rs->krns", values, eye)
        return full.reshape(outer * SUB, outer * SUB)

    first = np.concatenate([spread(np.cos(angle)), spread(-np.sin(angle))], axis=0)
    last = np.concatenate([spread(np.cos(angle)).T, spread(-np.sin(angle)).T], axis=1) / length
    inner = 2.0 * np.pi * np.outer(np.arange(INNER), np.arange(INNER)) / INNER
    c, s = np.cos(inner), np.sin(inner)
    middle = np.block([[c, s], [-s, c]])
    unmiddle = np.block([[c, -s], [s, c]])
    turn = 2.0 * np.pi * k1[None, :] * (SUB * np.arange(INNER // SUB))[:, None] / length
    scal_re = np.cos(turn).astype(np.float32)
    scal_im = np.sin(turn).astype(np.float32)
    return (
        const_halves(first),
        const_halves(last),
        const_halves(middle),
        const_halves(unmiddle),
        scal_re,
        scal_im,
    )


def forward_outer(x_ref, w_hi, w_lo, t_re, t_im, work):
    outer = x_ref.shape[0]
    lanes = x_ref.shape[2]

    def pair(i, carry):
        tiles = [
            x_ref[:, pl.ds(pl.multiple_of((2 * i + u) * SUB, SUB), SUB), :].reshape(
                outer * SUB, lanes
            )
            for u in range(2)
        ]
        out = mm3(w_hi[...], w_lo[...], jnp.concatenate(tiles, axis=1))
        for u in range(2):
            j = 2 * i + u
            row = pl.multiple_of(j * SUB, SUB)
            for k in range(outer):
                re = out[k * SUB : (k + 1) * SUB, u * lanes : (u + 1) * lanes]
                im = out[(outer + k) * SUB : (outer + k + 1) * SUB, u * lanes : (u + 1) * lanes]
                c, s = t_re[j, k], t_im[j, k]
                work[k, pl.ds(row, SUB), :] = re * c + im * s
                work[k, pl.ds(pl.multiple_of(INNER + row, SUB), SUB), :] = im * c - re * s
        return carry

    lax.fori_loop(0, INNER // SUB // 2, pair, 0)


def filter_kernel(w_hi, w_lo, b_hi, b_lo, t_re, t_im, filt, spec, x_ref, work):
    per = filt.shape[2] // INNER

    def turn(s, carry):
        for a in range(per):
            x_ref[per * s + a] = filt[s, :, a * INNER : (a + 1) * INNER].T
        return carry

    lax.fori_loop(0, filt.shape[0], turn, 0)
    forward_outer(x_ref, w_hi, w_lo, t_re, t_im, work)
    lanes = x_ref.shape[2]

    def inner(i, carry):
        both = jnp.concatenate([work[2 * i], work[2 * i + 1]], axis=1)
        out = mm3(b_hi[...], b_lo[...], both)
        spec[2 * i] = out[:, :lanes]
        spec[2 * i + 1] = out[:, lanes:]
        return carry

    lax.fori_loop(0, work.shape[0] // 2, inner, 0)


def signal_kernel(
    w_hi, w_lo, v_hi, v_lo, b_hi, b_lo, u_hi, u_lo, t_re, t_im, x_ref, spec, out_ref, work
):
    outer = x_ref.shape[0]
    lanes = x_ref.shape[2]
    forward_outer(x_ref, w_hi, w_lo, t_re, t_im, work)

    def inner(i, carry):
        both = jnp.concatenate([work[2 * i], work[2 * i + 1]], axis=1)
        x = mm3(b_hi[...], b_lo[...], both)
        h = jnp.concatenate([spec[2 * i], spec[2 * i + 1]], axis=1)
        x_re, x_im, h_re, h_im = x[:INNER], x[INNER:], h[:INNER], h[INNER:]
        z = jnp.concatenate([x_re * h_re - x_im * h_im, x_re * h_im + x_im * h_re], axis=0)
        y = mm3(u_hi[...], u_lo[...], z)
        work[2 * i] = y[:, :lanes]
        work[2 * i + 1] = y[:, lanes:]
        return carry

    lax.fori_loop(0, outer // 2, inner, 0)

    def back(i, carry):
        tiles = []
        for u in range(2):
            j = 2 * i + u
            row = pl.multiple_of(j * SUB, SUB)
            res, ims = [], []
            for k in range(outer):
                re = work[k, pl.ds(row, SUB), :]
                im = work[k, pl.ds(pl.multiple_of(INNER + row, SUB), SUB), :]
                c, s = t_re[j, k], t_im[j, k]
                res.append(re * c - im * s)
                ims.append(re * s + im * c)
            tiles.append(jnp.concatenate(res + ims, axis=0))
        out = mm3(v_hi[...], v_lo[...], jnp.concatenate(tiles, axis=1))
        for u in range(2):
            row = pl.multiple_of((2 * i + u) * SUB, SUB)
            part = out[:, u * lanes : (u + 1) * lanes].reshape(outer, SUB, lanes)
            out_ref[:, pl.ds(row, SUB), :] = part
        return carry

    lax.fori_loop(0, INNER // SUB // 2, back, 0)


def vmem_spec():
    return pl.BlockSpec(memory_space=pltpu.VMEM)


def smem_spec():
    return pl.BlockSpec(memory_space=pltpu.SMEM)


def filter_stage(filt, length):
    first, _, middle, _, t_re, t_im = long_tables(length)
    outer = length // INNER
    lanes = filt.shape[1]
    return pl.pallas_call(
        filter_kernel,
        in_specs=[vmem_spec()] * 4 + [smem_spec()] * 2 + [vmem_spec()],
        out_specs=vmem_spec(),
        out_shape=jax.ShapeDtypeStruct((outer, 2 * INNER, lanes), F32),
        scratch_shapes=[
            pltpu.VMEM((outer, INNER, lanes), F32),
            pltpu.VMEM((outer, 2 * INNER, lanes), F32),
        ],
        compiler_params=pltpu.CompilerParams(vmem_limit_bytes=VMEM_CAP),
        name="filter_stage",
    )(*first, *middle, t_re, t_im, filt)


def signal_stage(signal, spec):
    outer, _, lanes = signal.shape
    first, last, middle, unmiddle, t_re, t_im = long_tables(outer * INNER)
    return pl.pallas_call(
        signal_kernel,
        in_specs=[vmem_spec()] * 8 + [smem_spec()] * 2 + [vmem_spec()] * 2,
        out_specs=vmem_spec(),
        out_shape=jax.ShapeDtypeStruct(signal.shape, F32),
        scratch_shapes=[pltpu.VMEM((outer, 2 * INNER, lanes), F32)],
        compiler_params=pltpu.CompilerParams(vmem_limit_bytes=VMEM_CAP),
        name="signal_stage",
    )(*first, *last, *middle, *unmiddle, t_re, t_im, signal, spec)


def angle_table(row_count, col_count, modulus):
    product = (
        lax.iota(jnp.int32, row_count)[:, None] * lax.iota(jnp.int32, col_count)[None, :] % modulus
    )
    phase = product.astype(F32) * (2.0 * math.pi / modulus)
    return (jnp.cos(phase), jnp.sin(phase))


def plain_long_convolve(signal, kernel):
    high = lax.Precision.HIGHEST
    channels, length = signal.shape
    outer_len = 2 * length // INNER
    half_len = outer_len // 2
    cos_o, sin_o = angle_table(outer_len, half_len, outer_len)
    cos_t, sin_t = angle_table(outer_len, INNER, 2 * length)
    cos_i, sin_i = angle_table(INNER, INNER, INNER)
    stacked = jnp.concatenate([signal, kernel], axis=0).reshape(2 * channels, half_len, INNER)
    real = jnp.einsum("kn,cnq->ckq", cos_o, stacked, precision=high)
    imag = -jnp.einsum("kn,cnq->ckq", sin_o, stacked, precision=high)
    t_re = real * cos_t + imag * sin_t
    t_im = imag * cos_t - real * sin_t
    s_re = jnp.dot(t_re, cos_i, precision=high) + jnp.dot(t_im, sin_i, precision=high)
    s_im = jnp.dot(t_im, cos_i, precision=high) - jnp.dot(t_re, sin_i, precision=high)
    x_re, h_re, x_im, h_im = s_re[:channels], s_re[channels:], s_im[:channels], s_im[channels:]
    p_re = x_re * h_re - x_im * h_im
    p_im = x_re * h_im + x_im * h_re
    b_re = jnp.dot(p_re, cos_i, precision=high) - jnp.dot(p_im, sin_i, precision=high)
    b_im = jnp.dot(p_im, cos_i, precision=high) + jnp.dot(p_re, sin_i, precision=high)
    u_re = b_re * cos_t - b_im * sin_t
    u_im = b_re * sin_t + b_im * cos_t
    result = jnp.einsum("kn,ckq->cnq", cos_o, u_re, precision=high) - jnp.einsum(
        "kn,ckq->cnq", sin_o, u_im, precision=high
    )
    return result.reshape(channels, length) / (2.0 * length)


def hyena_kernel(place_ref, short_out, post, conv, out_ref, other_ref, mine_ref):
    parts = [conv[g] for g in range(conv.shape[0])]
    here = parts[0] if len(parts) == 1 else jnp.concatenate(parts, axis=1)
    result = short_out[...] + post[...] * here
    out_ref[...] = result
    step, half = pl.program_id(0), pl.num_programs(0) // 2

    @pl.when(step < half)
    def _():
        other_ref[...] = result

    @pl.when(step >= half)
    def _():
        mine_ref[...] = result


def hyena_stage(place, short_out, post, conv):
    length, width = short_out.shape
    _, _, group = conv.shape
    tile = max(group, 128)
    steps = width // tile
    half = steps // 2

    def col(i, place):
        return lax.rem((1 - place[1]) * half + i, steps)

    wide = pl.BlockSpec((length, tile), lambda i, place: (0, col(i, place)))
    return pl.pallas_call(
        hyena_kernel,
        grid_spec=pltpu.PrefetchScalarGridSpec(
            num_scalar_prefetch=1,
            grid=(steps,),
            in_specs=[
                wide,
                wide,
                pl.BlockSpec(
                    (tile // group, length, group), lambda i, place: (col(i, place), 0, 0)
                ),
            ],
            out_specs=[
                wide,
                pl.BlockSpec((length, tile), lambda i, place: (0, jnp.minimum(i, half - 1))),
                pl.BlockSpec((length, tile), lambda i, place: (0, jnp.maximum(i - half, 0))),
            ],
        ),
        out_shape=[
            jax.ShapeDtypeStruct((length, width), F32),
            jax.ShapeDtypeStruct((length, width // 2), F32),
            jax.ShapeDtypeStruct((length, width // 2), F32),
        ],
        name="hyena_stage",
    )(place, short_out, post, conv)


def load(ref):
    return ref[0] if len(ref.shape) == 3 else ref[...]


def ordered(refs, core):
    first = core == 0
    x = {name: load(ref) for name, ref in refs.items()}
    yield x["far"] + x["far_more"] if "far_more" in x else x["far"]
    yield jnp.where(first, x["near_mine"], x["near_other"])
    yield jnp.where(first, x["near_other"], x["near_mine"])
    yield jnp.where(first, x["mine"], x["other"])
    yield jnp.where(first, x["other"], x["mine"])


def fill_keys(k_cat, refs, core):
    for n, k in enumerate(ordered(refs, core)):
        hi, lo = halves(k.T)
        k_cat[n] = jnp.concatenate([hi, hi, lo], axis=0)


def fill_values(v_cat, refs, core):
    for n, v in enumerate(ordered(refs, core)):
        hi, lo = halves(v)
        v_cat[n] = jnp.concatenate([hi, lo], axis=1)


def query_cat(q_refs, turn):
    scale = math.log2(math.e) / math.sqrt(q_refs[0].shape[1])
    queries = jnp.where(turn == 0, q_refs[1][...], q_refs[0][...])
    hi, lo = halves(queries * scale)
    return jnp.concatenate([hi, lo, hi], axis=1)


def weigh(hi, lo, values):
    dim = values.shape[1] // 2
    both = mm(hi, values)
    return both[:, :dim] + both[:, dim:] + mm(lo, values[:, :dim])


def own_tiles(q_cat, k_own):
    length = q_cat.shape[0]
    tile = min(length, 256)
    for start in range(0, length, tile):
        stop = start + tile
        scores = mm(q_cat[start:stop], k_own[:, :stop])
        row = start + lax.broadcasted_iota(jnp.int32, (tile, stop), 0)
        col = lax.broadcasted_iota(jnp.int32, (tile, stop), 1)
        yield pl.ds(start, tile), stop, jnp.where(row >= col, scores, masked_low)


def attend_kernel(reach_ref, place_ref, *refs, head, names):
    count = len(names)
    q_refs = refs[:2]
    k_refs = dict(zip(names, refs[2 : 2 + count]))
    v_refs = dict(zip(names, refs[2 + count : 2 + 2 * count]))
    other_ref, mine_ref, k_cat, v_cat, top, total, acc = refs[2 + 2 * count :]
    turn = pl.program_id(0)
    core = place_ref[1]
    odd = jnp.where(turn == 0, 1 - core, core)

    @pl.when(turn == 0)
    def _():
        fill_keys(k_cat, k_refs, core)
        fill_values(v_cat, v_refs, core)

    q_cat = query_cat(q_refs, turn)
    reach = reach_ref[head]
    block = 2 * place_ref[0] + odd
    own = odd + REACH

    for rows, stop, scores in own_tiles(q_cat, k_cat[own]):
        best = jnp.max(scores, axis=1, keepdims=True)
        weight = jnp.exp2(scores - best)
        top[rows, :] = best
        total[rows, :] = jnp.sum(weight, axis=1, keepdims=True)
        acc[rows, :] = weigh(*halves(weight), v_cat[own, :stop, :])

    for distance in range(1, REACH + 1):

        @pl.when((distance <= reach) & (block >= distance))
        def _():
            slot = own - distance
            scores = mm(q_cat, k_cat[slot])
            old = top[...]
            best = jnp.maximum(old, jnp.max(scores, axis=1, keepdims=True))
            shrink = jnp.exp2(old - best)
            weight = jnp.exp2(scores - best)
            top[...] = best
            total[...] = total[...] * shrink + jnp.sum(weight, axis=1, keepdims=True)
            acc[...] = acc[...] * shrink + weigh(*halves(weight), v_cat[slot])

    result = acc[...] / total[...]

    @pl.when(turn == 0)
    def _():
        other_ref[...] = result

    @pl.when(turn == 1)
    def _():
        mine_ref[...] = result


def score_kernel(reach_ref, place_ref, *refs, head, names):
    count = len(names)
    q_refs = refs[:2]
    k_refs = dict(zip(names, refs[2 : 2 + count]))
    hi_ref, lo_ref, total_ref, k_cat, work, top = refs[2 + count :]
    turn = pl.program_id(0)
    core = place_ref[1]
    odd = jnp.where(turn == 0, 1 - core, core)

    @pl.when(turn == 0)
    def _():
        fill_keys(k_cat, k_refs, core)

    q_cat = query_cat(q_refs, turn)
    reach = reach_ref[head]
    block = 2 * place_ref[0] + odd
    own = odd + REACH
    length = work.shape[1]

    for rows, stop, scores in own_tiles(q_cat, k_cat[own]):
        top[rows, :] = jnp.max(scores, axis=1, keepdims=True)
        work[0, rows, :stop] = scores
        if stop < length:
            work[0, rows, stop:] = jnp.full((scores.shape[0], length - stop), masked_low, F32)

    def used(distance):
        return (distance <= reach) & (block >= distance)

    for distance in range(1, REACH + 1):

        @pl.when(used(distance))
        def _():
            scores = mm(q_cat, k_cat[own - distance])
            top[...] = jnp.maximum(top[...], jnp.max(scores, axis=1, keepdims=True))
            work[distance] = scores

    for distance in range(REACH + 1):

        def finish():
            weight = jnp.exp2(work[distance] - top[...])
            part = jnp.broadcast_to(jnp.sum(weight, axis=1, keepdims=True), total_ref.shape[1:])
            total_ref[0] = part if distance == 0 else total_ref[0] + part
            hi_ref[0, distance], lo_ref[0, distance] = halves(weight)

        if distance:
            pl.when(used(distance))(finish)
        else:
            finish()


def value_kernel(reach_ref, place_ref, *refs, head, names):
    hi_ref, lo_ref, total_ref = refs[:3]
    v_refs = dict(zip(names, refs[3:-4]))
    other_ref, mine_ref, v_cat, acc = refs[-4:]
    turn, distance = pl.program_id(0), pl.program_id(1)
    core = place_ref[1]
    odd = jnp.where(turn == 0, 1 - core, core)

    @pl.when((turn == 0) & (distance == 0))
    def _():
        fill_values(v_cat, v_refs, core)

    block = 2 * place_ref[0] + odd
    slot = odd + REACH - distance

    @pl.when(distance == 0)
    def _():
        acc[...] = weigh(hi_ref[0, 0], lo_ref[0, 0], v_cat[slot])

    @pl.when((distance > 0) & (distance <= reach_ref[head]) & (block >= distance))
    def _():
        acc[...] += weigh(hi_ref[0, 0], lo_ref[0, 0], v_cat[slot])

    @pl.when((distance == REACH) & (turn == 0))
    def _():
        other_ref[...] = acc[...] / total_ref[0]

    @pl.when((distance == REACH) & (turn == 1))
    def _():
        mine_ref[...] = acc[...] / total_ref[0]


def operand_specs(operands, head, length):
    def spec_of(x, lead):
        if lead is not None:
            return pl.BlockSpec((1, length, HEAD_DIM), lambda *_: (lead, 0, 0))
        at = head if x.shape[1] > HEAD_DIM else 0
        return pl.BlockSpec((length, HEAD_DIM), lambda *_: (0, at))

    return [spec_of(*x) for x in operands]


def attend_stage(reach, place, queries, keys, values, head):
    length = queries[0].shape[0]
    steps = REACH + 2
    operands = [(q, None) for q in queries] + list(keys.values()) + list(values.values())
    return pl.pallas_call(
        functools.partial(attend_kernel, head=head, names=tuple(keys)),
        grid_spec=pltpu.PrefetchScalarGridSpec(
            num_scalar_prefetch=2,
            grid=(2,),
            in_specs=operand_specs(operands, head, length),
            out_specs=[pl.BlockSpec((length, HEAD_DIM), lambda *_: (0, 0))] * 2,
            scratch_shapes=[
                pltpu.VMEM((steps, 3 * HEAD_DIM, length), BF16),
                pltpu.VMEM((steps, length, 2 * HEAD_DIM), BF16),
                pltpu.VMEM((length, 1), F32),
                pltpu.VMEM((length, 1), F32),
                pltpu.VMEM((length, HEAD_DIM), F32),
            ],
        ),
        out_shape=[jax.ShapeDtypeStruct((length, HEAD_DIM), F32)] * 2,
        compiler_params=pltpu.CompilerParams(vmem_limit_bytes=VMEM_CAP),
        name="attend_stage",
    )(reach, place, *[x for x, _ in operands])


def score_stage(reach, place, queries, keys, head):
    length = queries[0].shape[0]
    operands = [(q, None) for q in queries] + list(keys.values())
    big = (1, REACH + 1, length, length)
    return pl.pallas_call(
        functools.partial(score_kernel, head=head, names=tuple(keys)),
        grid_spec=pltpu.PrefetchScalarGridSpec(
            num_scalar_prefetch=2,
            grid=(2,),
            in_specs=operand_specs(operands, head, length),
            out_specs=[pl.BlockSpec(big, lambda i, *_: (i, 0, 0, 0))] * 2
            + [pl.BlockSpec((1, length, HEAD_DIM), lambda i, *_: (i, 0, 0))],
            scratch_shapes=[
                pltpu.VMEM((REACH + 2, 3 * HEAD_DIM, length), BF16),
                pltpu.VMEM(big[1:], F32),
                pltpu.VMEM((length, 1), F32),
            ],
        ),
        out_shape=[jax.ShapeDtypeStruct((2, *big[1:]), BF16)] * 2
        + [jax.ShapeDtypeStruct((2, length, HEAD_DIM), F32)],
        compiler_params=pltpu.CompilerParams(vmem_limit_bytes=VMEM_CAP),
        name="score_stage",
    )(reach, place, *[x for x, _ in operands])


def value_stage(reach, place, scored, values, head):
    hi, lo, total = scored
    length = hi.shape[2]
    operands = list(values.values())
    part = pl.BlockSpec((1, 1, length, length), lambda i, d, *_: (i, d, 0, 0))
    return pl.pallas_call(
        functools.partial(value_kernel, head=head, names=tuple(values)),
        grid_spec=pltpu.PrefetchScalarGridSpec(
            num_scalar_prefetch=2,
            grid=(2, REACH + 1),
            in_specs=[part, part, pl.BlockSpec((1, length, HEAD_DIM), lambda i, *_: (i, 0, 0))]
            + operand_specs(operands, head, length),
            out_specs=[pl.BlockSpec((length, HEAD_DIM), lambda *_: (0, 0))] * 2,
            scratch_shapes=[
                pltpu.VMEM((REACH + 2, length, 2 * HEAD_DIM), BF16),
                pltpu.VMEM((length, HEAD_DIM), F32),
            ],
        ),
        out_shape=[jax.ShapeDtypeStruct((length, HEAD_DIM), F32)] * 2,
        compiler_params=pltpu.CompilerParams(vmem_limit_bytes=VMEM_CAP),
        name="value_stage",
    )(reach, place, hi, lo, total, *[x for x, _ in operands])


def product_kernel(place_ref, *refs, sizes, added):
    count = len(sizes)
    a_groups, at = [], 0
    for size in sizes:
        a_groups.append(refs[at : at + size])
        at += size
    w_refs, rest = refs[at : at + 2 * count], refs[at + 2 * count :]
    out_ref, left = rest[-2:]

    @pl.when(pl.program_id(0) == 0)
    def _():
        apart = place_ref[0] ^ place_ref[2]
        for h in range(2):
            pieces = [sum((r[h] for r in group[1:]), group[0][h]) for group in a_groups]
            bit = 1
            while bit < count:
                flip = (apart & bit) != 0
                pieces = [jnp.where(flip, pieces[m ^ bit], pieces[m]) for m in range(count)]
                bit *= 2
            hi, lo = halves(jnp.concatenate(pieces, axis=1))
            left[h] = jnp.concatenate([hi, lo, hi], axis=1)

    out = None
    for h in range(2):
        hi, lo = halves(jnp.concatenate([r[...] for r in w_refs[h * count : (h + 1) * count]], axis=0))
        here = mm(left[h], jnp.concatenate([hi, hi, lo], axis=0))
        out = here if out is None else out + here
    out_ref[...] = rest[0][...] + out if added else out


def product_stage(place, pieces, weights, total):
    count = len(pieces)
    flat = [x for group in pieces for x in group]
    _, length, part = flat[0].shape
    width = weights[0][0].shape[1]
    tile = min(width, 256)
    a_spec = pl.BlockSpec((2, length, part), lambda i, place: (0, 0, 0))

    def w_spec(row):
        return pl.BlockSpec((part, tile), lambda i, place: (row, i))

    out_spec = pl.BlockSpec((length, tile), lambda i, place: (0, i))
    extra = [] if total is None else [total]
    return pl.pallas_call(
        functools.partial(
            product_kernel, sizes=tuple(len(g) for g in pieces), added=total is not None
        ),
        grid_spec=pltpu.PrefetchScalarGridSpec(
            num_scalar_prefetch=1,
            grid=(width // tile,),
            in_specs=[a_spec] * len(flat) + [w_spec(row) for _, row in weights] + [out_spec] * len(extra),
            out_specs=out_spec,
            scratch_shapes=[pltpu.VMEM((2, length, 3 * count * part), BF16)],
        ),
        out_shape=jax.ShapeDtypeStruct((length, width), F32),
        compiler_params=pltpu.CompilerParams(vmem_limit_bytes=VMEM_CAP),
        name="product_stage",
    )(place, *flat, *[w for w, _ in weights], *extra)


def shards(
    stream,
    short_gate_pre,
    short_gate_post,
    short_filter,
    long_gate_pre,
    long_gate_post,
    long_filter,
    queries,
    key_vectors,
    head_reach,
    out_weight,
):
    length, width = stream.shape
    taps = short_filter.shape[0]
    parts = lax.axis_size("seq")
    group = width // parts
    here = lax.axis_index("seq")
    chip, core = here // 2, here % 2
    half = width // 2
    heads_half = half // HEAD_DIM
    chips = parts // 2
    planes = lax.axis_size("chan")
    plane = lax.axis_index("chan")
    place = jnp.stack([chip, core, plane]).astype(jnp.int32)

    def send(x, pairs):
        return lax.ppermute(x, "seq", pairs)

    def shift(x, by):
        return send(x, [(i, i + by) for i in range(parts) if i + by < parts])

    def swap(x):
        return send(x, [(i, i ^ 1) for i in range(parts)])

    def both(x):
        cols = x.shape[1] // 2
        other = lax.dynamic_slice_in_dim(x, (1 - core) * cols, cols, 1)
        other = swap(other)
        return lax.dynamic_slice_in_dim(x, core * cols, cols, 1), other

    def cut(x, head):
        return x[:, head * HEAD_DIM : (head + 1) * HEAD_DIM]

    def own_of(mine, other):
        return {"mine": (mine, None), "other": (other, None)}

    def first_window(mine, other_out, other):
        both = range(0, parts, 2)
        near_mine = shift(cut(mine, 0), 2)
        crossed = [(c, c + 3) for c in both] + [(c + 1, c + 2) for c in both]
        near_other = send(cut(other_out, 0), [(i, j) for i, j in crossed if j < parts])
        far = send(cut(mine, 0), [(c + 1, c + 5) for c in both if c + 5 < parts])
        more = send(cut(other_out, 0), [(c + 1, c + 4) for c in both if c + 4 < parts])
        got = {"far": far, "far_more": more, "near_mine": near_mine, "near_other": near_other}
        return {k: (x, None) for k, x in got.items()} | own_of(mine, other)

    def later_windows(mine, other, heads):
        near = jnp.stack([cut(x, head) for head in heads for x in (mine, other)])
        far = jnp.stack([jnp.where(core == 0, cut(other, h), cut(mine, h)) for h in heads])
        near = shift(near, 2)
        far = shift(far, 4)
        return [
            {"far": (far, at), "near_mine": (near, 2 * at), "near_other": (near, 2 * at + 1)}
            | own_of(mine, other)
            for at in range(len(heads))
        ]

    tail = short_gate_pre[length - taps :] * stream[length - taps :]
    halo = shift(tail, 1)
    filt = long_filter.reshape(parts, group, length)
    filt = lax.all_to_all(filt, "seq", split_axis=0, concat_axis=0, tiled=True)
    short_out, long_in = short_stage(
        halo, stream, short_gate_pre, short_gate_post, short_filter, long_gate_pre, parts
    )
    signal = lax.all_to_all(long_in, "seq", split_axis=0, concat_axis=0, tiled=True)

    queries = both(queries)
    key_mine, key_other = both(key_vectors)
    whole = parts * length
    if group == 128 and whole <= 6144:
        spec = filter_stage(filt, whole)
        key_mine, key_other, spec = lax.optimization_barrier((key_mine, key_other, spec))
        conv = signal_stage(signal.reshape(whole // INNER, INNER, group), spec)
        conv = conv.reshape(parts, length, group)
    else:
        conv = plain_long_convolve(
            signal.reshape(whole, group).T, filt.transpose(1, 0, 2).reshape(group, whole)
        ).T.reshape(parts, length, group)
    reach = lax.dynamic_slice_in_dim(head_reach, core * heads_half, heads_half)
    key_windows = later_windows(key_mine, key_other, range(min(2, heads_half)))
    for n in range(2, heads_half):
        key_windows += later_windows(key_mine, key_other, [n])
    scored = score_stage(reach, place, queries, key_windows[0], 0)
    back = lax.all_to_all(conv, "seq", split_axis=0, concat_axis=0, tiled=True)
    hyena_out, value_out, value_mine = hyena_stage(place, short_out, long_gate_post, back)
    value_other = swap(value_out)

    mixed = None
    for n in range(heads_half):
        if n == 0:
            values = first_window(value_mine, value_out, value_other)
        else:
            values = later_windows(value_mine, value_other, [n])[0]
        if n == 0:
            other, mine = value_stage(reach, place, scored, values, n)
        else:
            other, mine = attend_stage(reach, place, queries, key_windows[n], values, n)
        if n == 0:
            out_weight, mine = lax.optimization_barrier((out_weight, mine))
            slots = [out_weight]
            relayed = chips == 4
            for m in range(1, chips - relayed):
                slots.append(send(out_weight, [(i, i ^ (2 * m)) for i in range(parts)]))
            if relayed:
                cut_at = out_weight.shape[0] // 2
                for m, piece in ((1, slots[1][:cut_at]), (2, slots[2][cut_at:])):
                    slots.append(send(piece, [(i, i ^ (6 - 2 * m)) for i in range(parts)]))
            partner = []
            for x in slots:
                partner.append(swap(x))
        piece = jnp.stack([mine, swap(other)])
        pieces = [[piece]]
        relays = planes == 4 and n < heads_half - 1
        for m in range(1, planes):
            pairs = [(i, i ^ m) for i in range(planes)]
            if relays and m > 1:
                pairs = [(0, 2), (3, 1)] if m == 2 else [(1, 2), (2, 1)]
            pieces.append([lax.ppermute(piece, "chan", pairs)])
        if relays:
            passed = {2: pieces[3][0], 3: pieces[2][0]}
            for m in (2, 3):
                pieces[m].append(lax.ppermute(passed[m], "chan", [(1, 0), (2, 3)]))
        if relayed:
            late = n * 2 // heads_half
            rows = [(0, n), (1, n), (2, n), (3 + late, n - late * (heads_half // 2))]
        else:
            rows = [(m, n) for m in range(chips)]
        weights = [(side[m], row) for side in (slots, partner) for m, row in rows]
        mixed = product_stage(place, pieces, weights, mixed)
    return (hyena_out, mixed)


def solution(mesh):
    return jax.shard_map(
        shards,
        mesh=mesh,
        in_specs=(
            P("seq", "chan"),
            P("seq", "chan"),
            P("seq", "chan"),
            P(None, "chan"),
            P("seq", "chan"),
            P("seq", "chan"),
            P("chan", "seq"),
            P("seq", "chan"),
            P("seq", "chan"),
            P("chan"),
            P("seq", "chan"),
        ),
        out_specs=(P("seq", "chan"), P("seq", "chan")),
        check_vma=False,
    )
```

```python
import functools
import math

import jax
import jax.numpy as jnp
import numpy as np
from jax import lax
from jax.experimental import pallas as pl
from jax.experimental.pallas import tpu as pltpu
from jax.sharding import PartitionSpec as P

HEAD_DIM = 128
REACH = 3
INNER = 128
SUB = 8
UNROLL = 2
SHORT_TILE = 512
HYENA_TILE = 256
PRODUCT_TILE = 256
ROW_TILE = 384


F32 = jnp.float32
BF16 = jnp.bfloat16
masked_low = -1e30
VMEM_CAP = 58 * 1024 * 1024


def halves(x):
    hi = x.astype(BF16)
    lo = (x - hi.astype(F32)).astype(BF16)
    return hi, lo


def const_halves(x):
    x = np.asarray(x, np.float32)
    hi = x.astype(BF16)
    lo = (x - hi.astype(np.float32)).astype(BF16)
    return hi, lo


def mm(a, b):
    return jnp.dot(a, b, preferred_element_type=F32)


def mm3(a_hi, a_lo, b):
    b_hi, b_lo = halves(b)
    left = jnp.concatenate([a_hi, a_lo, a_hi], axis=1)
    return mm(left, jnp.concatenate([b_hi, b_hi, b_lo], axis=0))


@functools.lru_cache(None)
def short_tables(taps):
    size = 2 * taps
    freq = 2.0 * np.pi * (np.arange(taps) + 0.5) / size
    angle = freq[:, None] * np.arange(size)[None, :]
    forward = np.concatenate([np.cos(angle), -np.sin(angle)], axis=0)
    back = angle[:, taps:].T
    inverse = np.concatenate([np.cos(back), -np.sin(back)], axis=1) * (2.0 / size)
    return const_halves(forward) + const_halves(inverse)


def short_kernel(
    f_hi, f_lo, g_hi, g_lo, halo, stream, pre, post, taps_ref, long_pre, out_ref, in_ref
):
    taps = taps_ref.shape[0]
    group = in_ref.shape[2]
    spec = mm3(f_hi[:, :taps], f_lo[:, :taps], taps_ref[...])
    h_re, h_im = spec[:taps], spec[taps:]
    before = halo[...]
    for block in range(stream.shape[0] // taps):
        rows = pl.ds(block * taps, taps)
        signal = stream[rows, :]
        here = pre[rows, :] * signal
        window = jnp.concatenate([before, here], axis=0)
        before = here
        x = mm3(f_hi[...], f_lo[...], window)
        x_re, x_im = x[:taps], x[taps:]
        z = jnp.concatenate([x_re * h_re - x_im * h_im, x_re * h_im + x_im * h_re], axis=0)
        conv = mm3(g_hi[...], g_lo[...], z)
        short_out = signal + post[rows, :] * conv
        out_ref[rows, :] = short_out
        long_in = long_pre[rows, :] * short_out
        for g in range(in_ref.shape[0]):
            in_ref[g, rows, :] = long_in[:, g * group : (g + 1) * group]


def short_stage(halo, stream, pre, post, taps, long_pre, parts):
    length, width = stream.shape
    taps_n = taps.shape[0]
    tile = min(width, SHORT_TILE)
    group = width // parts
    tables = short_tables(taps_n)
    wide = pl.BlockSpec((length, tile), lambda i: (0, i))
    narrow = pl.BlockSpec((taps_n, tile), lambda i: (0, i))
    fixed = [pl.BlockSpec(t.shape, lambda i: (0, 0)) for t in tables]
    return pl.pallas_call(
        short_kernel,
        grid=(width // tile,),
        in_specs=fixed + [narrow, wide, wide, wide, narrow, wide],
        out_specs=[wide, pl.BlockSpec((tile // group, length, group), lambda i: (i, 0, 0))],
        out_shape=[
            jax.ShapeDtypeStruct((length, width), F32),
            jax.ShapeDtypeStruct((parts, length, group), F32),
        ],
        compiler_params=pltpu.CompilerParams(vmem_limit_bytes=VMEM_CAP),
        name="short_stage",
    )(*tables, halo, stream, pre, post, taps, long_pre)


@functools.lru_cache(None)
def long_tables(length):
    outer = length // INNER
    k1 = np.arange(outer) + 0.25
    sub = np.arange(SUB)
    phase = (
        k1[:, None, None] * np.arange(outer)[None, :, None] / outer
        + k1[:, None, None] * sub[None, None, :] / length
    )
    angle = 2.0 * np.pi * phase
    eye = np.eye(SUB)

    def spread(values):
        full = np.einsum("knr,rs->krns", values, eye)
        return full.reshape(outer * SUB, outer * SUB)

    first = np.concatenate([spread(np.cos(angle)), spread(-np.sin(angle))], axis=0)
    last = np.concatenate([spread(np.cos(angle)).T, spread(-np.sin(angle)).T], axis=1) / length
    inner = 2.0 * np.pi * np.outer(np.arange(INNER), np.arange(INNER)) / INNER
    c, s = np.cos(inner), np.sin(inner)
    middle = np.block([[c, s], [-s, c]])
    unmiddle = np.block([[c, -s], [s, c]])
    turn = 2.0 * np.pi * k1[None, :] * (SUB * np.arange(INNER // SUB))[:, None] / length
    scal_re = np.cos(turn).astype(np.float32)
    scal_im = np.sin(turn).astype(np.float32)
    return (
        const_halves(first),
        const_halves(last),
        const_halves(middle),
        const_halves(unmiddle),
        scal_re,
        scal_im,
    )


def forward_outer(x_ref, w_hi, w_lo, t_re, t_im, work):
    outer = x_ref.shape[0]
    lanes = x_ref.shape[2]

    def pair(i, carry):
        tiles = [
            x_ref[:, pl.ds(pl.multiple_of((2 * i + u) * SUB, SUB), SUB), :].reshape(
                outer * SUB, lanes
            )
            for u in range(2)
        ]
        out = mm3(w_hi[...], w_lo[...], jnp.concatenate(tiles, axis=1))
        for u in range(2):
            j = 2 * i + u
            row = pl.multiple_of(j * SUB, SUB)
            for k in range(outer):
                re = out[k * SUB : (k + 1) * SUB, u * lanes : (u + 1) * lanes]
                im = out[(outer + k) * SUB : (outer + k + 1) * SUB, u * lanes : (u + 1) * lanes]
                c, s = t_re[j, k], t_im[j, k]
                work[k, pl.ds(row, SUB), :] = re * c + im * s
                work[k, pl.ds(pl.multiple_of(INNER + row, SUB), SUB), :] = im * c - re * s
        return carry

    lax.fori_loop(0, INNER // SUB // 2, pair, 0)


def filter_kernel(w_hi, w_lo, b_hi, b_lo, t_re, t_im, filt, spec, x_ref, work):
    per = filt.shape[2] // INNER

    def turn(s, carry):
        for a in range(per):
            x_ref[per * s + a] = filt[s, :, a * INNER : (a + 1) * INNER].T
        return carry

    lax.fori_loop(0, filt.shape[0], turn, 0)
    forward_outer(x_ref, w_hi, w_lo, t_re, t_im, work)
    lanes = x_ref.shape[2]

    rows = pl.ds(0, 2 * INNER)

    def inner(i, carry):
        for k in range(UNROLL):
            k = 2 * (UNROLL * i + k)
            both = jnp.concatenate([work[k, rows, :], work[k + 1, rows, :]], axis=1)
            out = mm3(b_hi[...], b_lo[...], both)
            spec[k] = out[:, :lanes]
            spec[k + 1] = out[:, lanes:]
        return carry

    lax.fori_loop(0, work.shape[0] // 2 // UNROLL, inner, 0)


def signal_kernel(
    w_hi, w_lo, v_hi, v_lo, b_hi, b_lo, u_hi, u_lo, t_re, t_im, x_ref, spec, out_ref, work
):
    outer = x_ref.shape[0]
    lanes = x_ref.shape[2]
    forward_outer(x_ref, w_hi, w_lo, t_re, t_im, work)

    rows = pl.ds(0, 2 * INNER)

    def inner(i, carry):
        ks = [2 * (UNROLL * i + k) for k in range(UNROLL)]
        xs = [
            mm3(b_hi[...], b_lo[...], jnp.concatenate([work[k, rows, :], work[k + 1, rows, :]], axis=1))
            for k in ks
        ]
        zs = []
        for k, x in zip(ks, xs):
            h = jnp.concatenate([spec[k], spec[k + 1]], axis=1)
            x_re, x_im, h_re, h_im = x[:INNER], x[INNER:], h[:INNER], h[INNER:]
            zs.append(
                jnp.concatenate([x_re * h_re - x_im * h_im, x_re * h_im + x_im * h_re], axis=0)
            )
        for k, z in zip(ks, zs):
            y = mm3(u_hi[...], u_lo[...], z)
            work[k, rows, :] = y[:, :lanes]
            work[k + 1, rows, :] = y[:, lanes:]
        return carry

    lax.fori_loop(0, outer // 2 // UNROLL, inner, 0)

    def back(i, carry):
        tiles = []
        for u in range(2):
            j = 2 * i + u
            row = pl.multiple_of(j * SUB, SUB)
            res, ims = [], []
            for k in range(outer):
                re = work[k, pl.ds(row, SUB), :]
                im = work[k, pl.ds(pl.multiple_of(INNER + row, SUB), SUB), :]
                c, s = t_re[j, k], t_im[j, k]
                res.append(re * c - im * s)
                ims.append(re * s + im * c)
            tiles.append(jnp.concatenate(res + ims, axis=0))
        out = mm3(v_hi[...], v_lo[...], jnp.concatenate(tiles, axis=1))
        for u in range(2):
            row = pl.multiple_of((2 * i + u) * SUB, SUB)
            part = out[:, u * lanes : (u + 1) * lanes].reshape(outer, SUB, lanes)
            out_ref[:, pl.ds(row, SUB), :] = part
        return carry

    lax.fori_loop(0, INNER // SUB // 2, back, 0)


def vmem_spec():
    return pl.BlockSpec(memory_space=pltpu.VMEM)


def smem_spec():
    return pl.BlockSpec(memory_space=pltpu.SMEM)


def filter_stage(filt, length):
    first, _, middle, _, t_re, t_im = long_tables(length)
    outer = length // INNER
    lanes = filt.shape[1]
    return pl.pallas_call(
        filter_kernel,
        in_specs=[vmem_spec()] * 4 + [smem_spec()] * 2 + [vmem_spec()],
        out_specs=vmem_spec(),
        out_shape=jax.ShapeDtypeStruct((outer, 2 * INNER, lanes), F32),
        scratch_shapes=[
            pltpu.VMEM((outer, INNER, lanes), F32),
            pltpu.VMEM((outer, 2 * INNER, lanes), F32),
        ],
        compiler_params=pltpu.CompilerParams(vmem_limit_bytes=VMEM_CAP),
        name="filter_stage",
    )(*first, *middle, t_re, t_im, filt)


def signal_stage(signal, spec):
    outer, _, lanes = signal.shape
    first, last, middle, unmiddle, t_re, t_im = long_tables(outer * INNER)
    return pl.pallas_call(
        signal_kernel,
        in_specs=[vmem_spec()] * 8 + [smem_spec()] * 2 + [vmem_spec()] * 2,
        out_specs=vmem_spec(),
        out_shape=jax.ShapeDtypeStruct(signal.shape, F32),
        scratch_shapes=[pltpu.VMEM((outer, 2 * INNER, lanes), F32)],
        compiler_params=pltpu.CompilerParams(vmem_limit_bytes=VMEM_CAP),
        name="signal_stage",
    )(*first, *last, *middle, *unmiddle, t_re, t_im, signal, spec)


def angle_table(row_count, col_count, modulus):
    product = (
        lax.iota(jnp.int32, row_count)[:, None] * lax.iota(jnp.int32, col_count)[None, :] % modulus
    )
    phase = product.astype(F32) * (2.0 * math.pi / modulus)
    return (jnp.cos(phase), jnp.sin(phase))


def plain_long_convolve(signal, kernel):
    high = lax.Precision.HIGHEST
    channels, length = signal.shape
    outer_len = 2 * length // INNER
    half_len = outer_len // 2
    cos_o, sin_o = angle_table(outer_len, half_len, outer_len)
    cos_t, sin_t = angle_table(outer_len, INNER, 2 * length)
    cos_i, sin_i = angle_table(INNER, INNER, INNER)
    stacked = jnp.concatenate([signal, kernel], axis=0).reshape(2 * channels, half_len, INNER)
    real = jnp.einsum("kn,cnq->ckq", cos_o, stacked, precision=high)
    imag = -jnp.einsum("kn,cnq->ckq", sin_o, stacked, precision=high)
    t_re = real * cos_t + imag * sin_t
    t_im = imag * cos_t - real * sin_t
    s_re = jnp.dot(t_re, cos_i, precision=high) + jnp.dot(t_im, sin_i, precision=high)
    s_im = jnp.dot(t_im, cos_i, precision=high) - jnp.dot(t_re, sin_i, precision=high)
    x_re, h_re, x_im, h_im = s_re[:channels], s_re[channels:], s_im[:channels], s_im[channels:]
    p_re = x_re * h_re - x_im * h_im
    p_im = x_re * h_im + x_im * h_re
    b_re = jnp.dot(p_re, cos_i, precision=high) - jnp.dot(p_im, sin_i, precision=high)
    b_im = jnp.dot(p_im, cos_i, precision=high) + jnp.dot(p_re, sin_i, precision=high)
    u_re = b_re * cos_t - b_im * sin_t
    u_im = b_re * sin_t + b_im * cos_t
    result = jnp.einsum("kn,ckq->cnq", cos_o, u_re, precision=high) - jnp.einsum(
        "kn,ckq->cnq", sin_o, u_im, precision=high
    )
    return result.reshape(channels, length) / (2.0 * length)


def hyena_kernel(place_ref, short_out, post, conv, out_ref, other_ref, mine_ref):
    parts = [conv[g] for g in range(conv.shape[0])]
    here = parts[0] if len(parts) == 1 else jnp.concatenate(parts, axis=1)
    result = short_out[...] + post[...] * here
    out_ref[...] = result
    step, half = pl.program_id(0), pl.num_programs(0) // 2

    @pl.when(step < half)
    def _():
        other_ref[...] = result

    @pl.when(step >= half)
    def _():
        mine_ref[...] = result


def hyena_stage(place, short_out, post, conv):
    length, width = short_out.shape
    _, _, group = conv.shape
    tile = max(group, HYENA_TILE)
    steps = width // tile
    half = steps // 2

    def col(i, place):
        return lax.rem((1 - place[1]) * half + i, steps)

    wide = pl.BlockSpec((length, tile), lambda i, place: (0, col(i, place)))
    return pl.pallas_call(
        hyena_kernel,
        grid_spec=pltpu.PrefetchScalarGridSpec(
            num_scalar_prefetch=1,
            grid=(steps,),
            in_specs=[
                wide,
                wide,
                pl.BlockSpec(
                    (tile // group, length, group), lambda i, place: (col(i, place), 0, 0)
                ),
            ],
            out_specs=[
                wide,
                pl.BlockSpec((length, tile), lambda i, place: (0, jnp.minimum(i, half - 1))),
                pl.BlockSpec((length, tile), lambda i, place: (0, jnp.maximum(i - half, 0))),
            ],
        ),
        out_shape=[
            jax.ShapeDtypeStruct((length, width), F32),
            jax.ShapeDtypeStruct((length, width // 2), F32),
            jax.ShapeDtypeStruct((length, width // 2), F32),
        ],
        name="hyena_stage",
    )(place, short_out, post, conv)


def load(ref):
    return ref[0] if len(ref.shape) == 3 else ref[...]


def ordered(refs, core):
    first = core == 0
    x = {name: load(ref) for name, ref in refs.items()}
    yield x["far"] + x["far_more"] if "far_more" in x else x["far"]
    if "even" in x:
        yield x["even"]
        yield x["odd"] + x["relay"] if "relay" in x else x["odd"]
    else:
        yield jnp.where(first, x["near_mine"], x["near_other"])
        yield jnp.where(first, x["near_other"], x["near_mine"])
    yield jnp.where(first, x["mine"], x["other"])
    yield jnp.where(first, x["other"], x["mine"])


def fill_keys(k_cat, refs, core):
    for n, k in enumerate(ordered(refs, core)):
        hi, lo = halves(k.T)
        k_cat[n] = jnp.concatenate([hi, hi, lo], axis=0)


def fill_values(v_cat, refs, core):
    for n, v in enumerate(ordered(refs, core)):
        hi, lo = halves(v)
        v_cat[n] = jnp.concatenate([hi, lo], axis=1)


def query_cat(q_refs, turn):
    scale = math.log2(math.e) / math.sqrt(q_refs[0].shape[1])
    queries = jnp.where(turn == 0, q_refs[1][...], q_refs[0][...])
    hi, lo = halves(queries * scale)
    return jnp.concatenate([hi, lo, hi], axis=1)


def weigh(hi, lo, values):
    dim = values.shape[1] // 2
    both = mm(hi, values)
    return both[:, :dim] + both[:, dim:] + mm(lo, values[:, :dim])


def own_tiles(q_cat, k_own):
    length = q_cat.shape[0]
    tile = min(length, 256)
    for start in range(0, length, tile):
        stop = start + tile
        scores = mm(q_cat[start:stop], k_own[:, :stop])
        row = start + lax.broadcasted_iota(jnp.int32, (tile, stop), 0)
        col = lax.broadcasted_iota(jnp.int32, (tile, stop), 1)
        yield pl.ds(start, tile), stop, jnp.where(row >= col, scores, masked_low)


def attend_kernel(reach_ref, place_ref, *refs, head, names):
    count = len(names)
    q_refs = refs[:2]
    k_refs = dict(zip(names, refs[2 : 2 + count]))
    v_refs = dict(zip(names, refs[2 + count : 2 + 2 * count]))
    other_ref, mine_ref, k_cat, v_cat, top, total, acc = refs[2 + 2 * count :]
    turn = pl.program_id(0)
    core = place_ref[1]
    odd = jnp.where(turn == 0, 1 - core, core)

    @pl.when(turn == 0)
    def _():
        fill_keys(k_cat, k_refs, core)
        fill_values(v_cat, v_refs, core)

    q_cat = query_cat(q_refs, turn)
    reach = reach_ref[head]
    block = 2 * place_ref[0] + odd
    own = odd + REACH

    for rows, stop, scores in own_tiles(q_cat, k_cat[own]):
        best = jnp.max(scores, axis=1, keepdims=True)
        weight = jnp.exp2(scores - best)
        top[rows, :] = best
        total[rows, :] = jnp.sum(weight, axis=1, keepdims=True)
        acc[rows, :] = weigh(*halves(weight), v_cat[own, :stop, :])

    for distance in range(1, REACH + 1):

        @pl.when((distance <= reach) & (block >= distance))
        def _():
            slot = own - distance
            length = q_cat.shape[0]
            tile = min(length, ROW_TILE)
            for start in range(0, length, tile):
                rows = pl.ds(start, tile)
                scores = mm(q_cat[start : start + tile], k_cat[slot])
                old = top[rows, :]
                best = jnp.maximum(old, jnp.max(scores, axis=1, keepdims=True))
                shrink = jnp.exp2(old - best)
                weight = jnp.exp2(scores - best)
                top[rows, :] = best
                total[rows, :] = total[rows, :] * shrink + jnp.sum(weight, axis=1, keepdims=True)
                acc[rows, :] = acc[rows, :] * shrink + weigh(*halves(weight), v_cat[slot])

    result = acc[...] / total[...]

    @pl.when(turn == 0)
    def _():
        other_ref[...] = result

    @pl.when(turn == 1)
    def _():
        mine_ref[...] = result


def score_kernel(reach_ref, place_ref, *refs, head, names):
    count = len(names)
    q_refs = refs[:2]
    k_refs = dict(zip(names, refs[2 : 2 + count]))
    hi_ref, lo_ref, total_ref, k_cat, work, top = refs[2 + count :]
    turn = pl.program_id(0)
    core = place_ref[1]
    odd = jnp.where(turn == 0, 1 - core, core)

    @pl.when(turn == 0)
    def _():
        fill_keys(k_cat, k_refs, core)

    q_cat = query_cat(q_refs, turn)
    reach = reach_ref[head]
    block = 2 * place_ref[0] + odd
    own = odd + REACH
    length = work.shape[1]

    for rows, stop, scores in own_tiles(q_cat, k_cat[own]):
        top[rows, :] = jnp.max(scores, axis=1, keepdims=True)
        work[0, rows, :stop] = scores
        if stop < length:
            work[0, rows, stop:] = jnp.full((scores.shape[0], length - stop), masked_low, F32)

    def used(distance):
        return (distance <= reach) & (block >= distance)

    for distance in range(1, REACH + 1):

        @pl.when(used(distance))
        def _():
            scores = mm(q_cat, k_cat[own - distance])
            top[...] = jnp.maximum(top[...], jnp.max(scores, axis=1, keepdims=True))
            work[distance] = scores

    for distance in range(REACH + 1):

        def finish():
            weight = jnp.exp2(work[distance] - top[...])
            part = jnp.broadcast_to(jnp.sum(weight, axis=1, keepdims=True), total_ref.shape[1:])
            total_ref[0] = part if distance == 0 else total_ref[0] + part
            hi_ref[0, distance], lo_ref[0, distance] = halves(weight)

        if distance:
            pl.when(used(distance))(finish)
        else:
            finish()


def value_kernel(reach_ref, place_ref, *refs, head, names):
    hi_ref, lo_ref, total_ref = refs[:3]
    v_refs = dict(zip(names, refs[3:-4]))
    other_ref, mine_ref, v_cat, acc = refs[-4:]
    turn, distance = pl.program_id(0), pl.program_id(1)
    core = place_ref[1]
    odd = jnp.where(turn == 0, 1 - core, core)

    @pl.when((turn == 0) & (distance == 0))
    def _():
        fill_values(v_cat, v_refs, core)

    block = 2 * place_ref[0] + odd
    slot = odd + REACH - distance

    @pl.when(distance == 0)
    def _():
        acc[...] = weigh(hi_ref[0, 0], lo_ref[0, 0], v_cat[slot])

    @pl.when((distance > 0) & (distance <= reach_ref[head]) & (block >= distance))
    def _():
        acc[...] += weigh(hi_ref[0, 0], lo_ref[0, 0], v_cat[slot])

    @pl.when((distance == REACH) & (turn == 0))
    def _():
        other_ref[...] = acc[...] / total_ref[0]

    @pl.when((distance == REACH) & (turn == 1))
    def _():
        mine_ref[...] = acc[...] / total_ref[0]


def operand_specs(operands, head, length):
    def spec_of(x, lead):
        if lead is not None:
            return pl.BlockSpec((1, length, HEAD_DIM), lambda *_: (lead, 0, 0))
        at = head if x.shape[1] > HEAD_DIM else 0
        return pl.BlockSpec((length, HEAD_DIM), lambda *_: (0, at))

    return [spec_of(*x) for x in operands]


def attend_stage(reach, place, queries, keys, values, head):
    length = queries[0].shape[0]
    steps = REACH + 2
    operands = [(q, None) for q in queries] + list(keys.values()) + list(values.values())
    return pl.pallas_call(
        functools.partial(attend_kernel, head=head, names=tuple(keys)),
        grid_spec=pltpu.PrefetchScalarGridSpec(
            num_scalar_prefetch=2,
            grid=(2,),
            in_specs=operand_specs(operands, head, length),
            out_specs=[pl.BlockSpec((length, HEAD_DIM), lambda *_: (0, 0))] * 2,
            scratch_shapes=[
                pltpu.VMEM((steps, 3 * HEAD_DIM, length), BF16),
                pltpu.VMEM((steps, length, 2 * HEAD_DIM), BF16),
                pltpu.VMEM((length, 1), F32),
                pltpu.VMEM((length, 1), F32),
                pltpu.VMEM((length, HEAD_DIM), F32),
            ],
        ),
        out_shape=[jax.ShapeDtypeStruct((length, HEAD_DIM), F32)] * 2,
        compiler_params=pltpu.CompilerParams(vmem_limit_bytes=VMEM_CAP),
        name="attend_stage",
    )(reach, place, *[x for x, _ in operands])


def score_stage(reach, place, queries, keys, head):
    length = queries[0].shape[0]
    operands = [(q, None) for q in queries] + list(keys.values())
    big = (1, REACH + 1, length, length)
    return pl.pallas_call(
        functools.partial(score_kernel, head=head, names=tuple(keys)),
        grid_spec=pltpu.PrefetchScalarGridSpec(
            num_scalar_prefetch=2,
            grid=(2,),
            in_specs=operand_specs(operands, head, length),
            out_specs=[pl.BlockSpec(big, lambda i, *_: (i, 0, 0, 0))] * 2
            + [pl.BlockSpec((1, length, HEAD_DIM), lambda i, *_: (i, 0, 0))],
            scratch_shapes=[
                pltpu.VMEM((REACH + 2, 3 * HEAD_DIM, length), BF16),
                pltpu.VMEM(big[1:], F32),
                pltpu.VMEM((length, 1), F32),
            ],
        ),
        out_shape=[jax.ShapeDtypeStruct((2, *big[1:]), BF16)] * 2
        + [jax.ShapeDtypeStruct((2, length, HEAD_DIM), F32)],
        compiler_params=pltpu.CompilerParams(vmem_limit_bytes=VMEM_CAP),
        name="score_stage",
    )(reach, place, *[x for x, _ in operands])


def value_stage(reach, place, scored, values, head):
    hi, lo, total = scored
    length = hi.shape[2]
    operands = list(values.values())
    part = pl.BlockSpec((1, 1, length, length), lambda i, d, *_: (i, d, 0, 0))
    return pl.pallas_call(
        functools.partial(value_kernel, head=head, names=tuple(values)),
        grid_spec=pltpu.PrefetchScalarGridSpec(
            num_scalar_prefetch=2,
            grid=(2, REACH + 1),
            in_specs=[part, part, pl.BlockSpec((1, length, HEAD_DIM), lambda i, *_: (i, 0, 0))]
            + operand_specs(operands, head, length),
            out_specs=[pl.BlockSpec((length, HEAD_DIM), lambda *_: (0, 0))] * 2,
            scratch_shapes=[
                pltpu.VMEM((REACH + 2, length, 2 * HEAD_DIM), BF16),
                pltpu.VMEM((length, HEAD_DIM), F32),
            ],
        ),
        out_shape=[jax.ShapeDtypeStruct((length, HEAD_DIM), F32)] * 2,
        compiler_params=pltpu.CompilerParams(vmem_limit_bytes=VMEM_CAP),
        name="value_stage",
    )(reach, place, hi, lo, total, *[x for x, _ in operands])


def product_kernel(place_ref, *refs, sizes, added):
    count = len(sizes)
    a_groups, at = [], 0
    for size in sizes:
        a_groups.append(refs[at : at + size])
        at += size
    w_refs, rest = refs[at : at + 2 * count], refs[at + 2 * count :]
    out_ref, left = rest[-2:]

    @pl.when(pl.program_id(0) == 0)
    def _():
        apart = place_ref[0] ^ place_ref[2]
        for h in range(2):
            pieces = [sum((r[h] for r in group[1:]), group[0][h]) for group in a_groups]
            bit = 1
            while bit < count:
                flip = (apart & bit) != 0
                pieces = [jnp.where(flip, pieces[m ^ bit], pieces[m]) for m in range(count)]
                bit *= 2
            hi, lo = halves(jnp.concatenate(pieces, axis=1))
            left[h] = jnp.concatenate([hi, lo, hi], axis=1)

    out = None
    for h in range(2):
        hi, lo = halves(jnp.concatenate([r[...] for r in w_refs[h * count : (h + 1) * count]], axis=0))
        here = mm(left[h], jnp.concatenate([hi, hi, lo], axis=0))
        out = here if out is None else out + here
    out_ref[...] = rest[0][...] + out if added else out


def product_stage(place, pieces, weights, total):
    count = len(pieces)
    flat = [x for group in pieces for x in group]
    _, length, part = flat[0].shape
    width = weights[0][0].shape[1]
    tile = min(width, PRODUCT_TILE)
    a_spec = pl.BlockSpec((2, length, part), lambda i, place: (0, 0, 0))

    def w_spec(row):
        return pl.BlockSpec((part, tile), lambda i, place: (row, i))

    out_spec = pl.BlockSpec((length, tile), lambda i, place: (0, i))
    extra = [] if total is None else [total]
    return pl.pallas_call(
        functools.partial(
            product_kernel, sizes=tuple(len(g) for g in pieces), added=total is not None
        ),
        grid_spec=pltpu.PrefetchScalarGridSpec(
            num_scalar_prefetch=1,
            grid=(width // tile,),
            in_specs=[a_spec] * len(flat) + [w_spec(row) for _, row in weights] + [out_spec] * len(extra),
            out_specs=out_spec,
            scratch_shapes=[pltpu.VMEM((2, length, 3 * count * part), BF16)],
        ),
        out_shape=jax.ShapeDtypeStruct((length, width), F32),
        compiler_params=pltpu.CompilerParams(vmem_limit_bytes=VMEM_CAP),
        name="product_stage",
    )(place, *flat, *[w for w, _ in weights], *extra)


def shards(
    stream,
    short_gate_pre,
    short_gate_post,
    short_filter,
    long_gate_pre,
    long_gate_post,
    long_filter,
    queries,
    key_vectors,
    head_reach,
    out_weight,
):
    length, width = stream.shape
    taps = short_filter.shape[0]
    parts = lax.axis_size("seq")
    group = width // parts
    here = lax.axis_index("seq")
    chip, core = here // 2, here % 2
    half = width // 2
    heads_half = half // HEAD_DIM
    chips = parts // 2
    planes = lax.axis_size("chan")
    plane = lax.axis_index("chan")
    place = jnp.stack([chip, core, plane]).astype(jnp.int32)

    def send(x, pairs):
        return lax.ppermute(x, "seq", pairs)

    def shift(x, by):
        return send(x, [(i, i + by) for i in range(parts) if i + by < parts])

    def swap(x):
        return send(x, [(i, i ^ 1) for i in range(parts)])

    def both(x):
        cols = x.shape[1] // 2
        other = lax.dynamic_slice_in_dim(x, (1 - core) * cols, cols, 1)
        other = swap(other)
        return lax.dynamic_slice_in_dim(x, core * cols, cols, 1), other

    def cut(x, head):
        return x[:, head * HEAD_DIM : (head + 1) * HEAD_DIM]

    def own_of(mine, other):
        return {"mine": (mine, None), "other": (other, None)}

    def first_window(mine, other_out, other):
        both = range(0, parts, 2)
        near_mine = shift(cut(mine, 0), 2)
        crossed = [(c, c + 3) for c in both] + [(c + 1, c + 2) for c in both]
        near_other = send(cut(other_out, 0), [(i, j) for i, j in crossed if j < parts])
        far = send(cut(mine, 0), [(c + 1, c + 5) for c in both if c + 5 < parts])
        more = send(cut(other_out, 0), [(c + 1, c + 4) for c in both if c + 4 < parts])
        got = {"far": far, "far_more": more, "near_mine": near_mine, "near_other": near_other}
        return {k: (x, None) for k, x in got.items()} | own_of(mine, other)

    def later_windows(mine, other, heads):
        near = jnp.stack([cut(x, head) for head in heads for x in (mine, other)])
        far = jnp.stack([jnp.where(core == 0, cut(other, h), cut(mine, h)) for h in heads])
        near = shift(near, 2)
        far = shift(far, 4)
        return [
            {"far": (far, at), "near_mine": (near, 2 * at), "near_other": (near, 2 * at + 1)}
            | own_of(mine, other)
            for at in range(len(heads))
        ]

    def joint_windows(key_pair, value_pair, head):
        first = core == 0
        pairs = [[cut(x, head) for x in pair] for pair in (key_pair, value_pair)]
        odd = jnp.stack([jnp.where(first, other, mine) for mine, other in pairs])
        even = jnp.stack([jnp.where(first, mine, other) for mine, other in pairs])
        got = {}
        got["far"] = shift(odd, 4)
        got["even"] = shift(even, 2)
        direct = (0, 1, 4, 5) if chips == 4 else range(parts - 2)
        got["odd"] = send(odd, [(i, i + 2) for i in direct])
        if chips == 4:
            got["relay"] = send(got["far"], [(6, 4), (7, 5)])
        return [
            {name: (x, at) for name, x in got.items()} | own_of(*pair)
            for at, pair in enumerate((key_pair, value_pair))
        ]

    tail = short_gate_pre[length - taps :] * stream[length - taps :]
    halo = shift(tail, 1)
    filt = long_filter.reshape(parts, group, length)
    filt = lax.all_to_all(filt, "seq", split_axis=0, concat_axis=0, tiled=True)
    short_out, long_in = short_stage(
        halo, stream, short_gate_pre, short_gate_post, short_filter, long_gate_pre, parts
    )
    signal = lax.all_to_all(long_in, "seq", split_axis=0, concat_axis=0, tiled=True)

    queries = both(queries)
    key_mine, key_other = both(key_vectors)
    whole = parts * length
    if group == 128 and whole <= 6144:
        spec = filter_stage(filt, whole)
        key_mine, key_other, spec = lax.optimization_barrier((key_mine, key_other, spec))
        conv = signal_stage(signal.reshape(whole // INNER, INNER, group), spec)
        conv = conv.reshape(parts, length, group)
    else:
        conv = plain_long_convolve(
            signal.reshape(whole, group).T, filt.transpose(1, 0, 2).reshape(group, whole)
        ).T.reshape(parts, length, group)
    reach = lax.dynamic_slice_in_dim(head_reach, core * heads_half, heads_half)
    keys = later_windows(key_mine, key_other, [0])[0]
    scored = score_stage(reach, place, queries, keys, 0)
    back = lax.all_to_all(conv, "seq", split_axis=0, concat_axis=0, tiled=True)
    hyena_out, value_out, value_mine = hyena_stage(place, short_out, long_gate_post, back)
    value_other = swap(value_out)

    mixed = None
    for n in range(heads_half):
        if n == 0:
            values = first_window(value_mine, value_out, value_other)
        else:
            keys, values = joint_windows((key_mine, key_other), (value_mine, value_other), n)
        if n == 0:
            other, mine = value_stage(reach, place, scored, values, n)
        else:
            other, mine = attend_stage(reach, place, queries, keys, values, n)
        if n == 0:
            out_weight, mine = lax.optimization_barrier((out_weight, mine))
            slots = [out_weight]
            relayed = chips == 4
            for m in range(1, chips - relayed):
                slots.append(send(out_weight, [(i, i ^ (2 * m)) for i in range(parts)]))
            if relayed:
                cut_at = out_weight.shape[0] // 2
                for m, piece in ((1, slots[1][:cut_at]), (2, slots[2][cut_at:])):
                    slots.append(send(piece, [(i, i ^ (6 - 2 * m)) for i in range(parts)]))
            partner = []
            for x in slots:
                partner.append(swap(x))
        piece = jnp.stack([mine, swap(other)])
        pieces = [[piece]]
        relays = planes == 4 and 0 < n < heads_half - 1
        for m in range(1, planes):
            pairs = [(i, i ^ m) for i in range(planes)]
            if relays and m > 1:
                pairs = [(0, 2), (3, 1)] if m == 2 else [(1, 2), (2, 1)]
            pieces.append([lax.ppermute(piece, "chan", pairs)])
        if relays:
            passed = {2: pieces[3][0], 3: pieces[2][0]}
            for m in (2, 3):
                pieces[m].append(lax.ppermute(passed[m], "chan", [(1, 0), (2, 3)]))
        if relayed:
            late = n * 2 // heads_half
            rows = [(0, n), (1, n), (2, n), (3 + late, n - late * (heads_half // 2))]
        else:
            rows = [(m, n) for m in range(chips)]
        weights = [(side[m], row) for side in (slots, partner) for m, row in rows]
        mixed = product_stage(place, pieces, weights, mixed)
    return (hyena_out, mixed)


def solution(mesh):
    return jax.shard_map(
        shards,
        mesh=mesh,
        in_specs=(
            P("seq", "chan"),
            P("seq", "chan"),
            P("seq", "chan"),
            P(None, "chan"),
            P("seq", "chan"),
            P("seq", "chan"),
            P("chan", "seq"),
            P("seq", "chan"),
            P("seq", "chan"),
            P("chan"),
            P("seq", "chan"),
        ),
        out_specs=(P("seq", "chan"), P("seq", "chan")),
        check_vma=False,
    )
```
